512 devices in a mesh: dp: 32 (over y_lo, z), owner: 16 (over x, y_hi, core).
Axes of the slice: x: 4, y: 8 (y_hi: 2, y_lo: 4; y = y_hi * 4 + y_lo), z: 8, core: 2. Of those that a mesh axis runs over, the one named last changes fastest.
Arguments:
- gradients: bfloat16 [32, 16, 512, 512], P('dp', 'owner'), may hold values from -600 to 600
- block_layer: int32 [16], P('owner'), may hold values from 0 to 3
Outputs:
- update: bfloat16 [16, 512, 512], P('owner', 'dp')
The draws below stay inside these ranges and needn't reach their ends.
All inputs are finite; a program needn't handle non-finite values.
Results may differ from the reference program's by a relative error of at most 0.0062.
Values may be sent and summed in bfloat16 or wider, within the bound.
A program may use at most 64 MiB of HBM per device.

```python
import math
import jax
import jax.numpy as jnp
from jax import lax

B = 512
LAYERS = 4
ITERS = 3
NBLK = 16
N_DP = 32


def draw_gradients(key, part):
    first_key = jax.random.fold_in(jax.random.fold_in(key, 11), 0)
    third_key = jax.random.fold_in(jax.random.fold_in(key, 11), 2)
    fourth_key = jax.random.fold_in(jax.random.fold_in(key, 11), 3)
    fifth_key = jax.random.fold_in(jax.random.fold_in(key, 11), 4)
    scales = jnp.exp(jax.random.uniform(first_key, (N_DP, NBLK, 1, 1), jnp.float32, 0.0, math.log(10.0)))
    heavy = jax.random.randint(fourth_key, (1, NBLK, 1, 1), 0, N_DP)
    replica_ids = jnp.arange(N_DP, dtype=jnp.int32)[:, None, None, None]
    scales = jnp.where(replica_ids == heavy, 25.0, scales)
    row_place = jnp.arange(B, dtype=jnp.float32)[None, None, :, None] / float(B - 1)
    jitter = jnp.exp(jax.random.uniform(fifth_key, (1, NBLK, B, 1), jnp.float32, math.log(0.8), math.log(1.25)))
    ramp = jnp.exp(0.5 * math.log(10.0) * row_place) * jitter
    values = jnp.clip(jax.random.normal(third_key, (N_DP, NBLK, B, B), jnp.float32), -6.0, 6.0)
    return (scales * ramp * values).astype(jnp.bfloat16)


def with_ends(array, stream_key, low, high):
    extent = array.shape
    place = [jax.random.randint(jax.random.fold_in(stream_key, axis), (), 0, extent[axis]) for axis in range(len(extent))]
    array = array.at[tuple(place)].set(low)
    longest = extent.index(max(extent))
    place[longest] = (place[longest] + 1) % extent[longest]
    return array.at[tuple(place)].set(high)


def setup_inputs(seed: int = 0) -> dict:
    arg_keys = jax.random.split(jax.random.key(seed), 3)
    return {
        "gradients": draw_gradients(jax.random.fold_in(arg_keys[2], 71), 0),
        "block_layer": with_ends(jax.random.randint(arg_keys[1], (NBLK,), 0, LAYERS), jax.random.fold_in(arg_keys[1], 1), 0, LAYERS - 1).astype(jnp.int32),
    }


def inverse_root(statistic):
    size_b = statistic.shape[0]
    identity = jnp.eye(size_b, dtype=jnp.float32)
    ridge_term = 0.01 * jnp.trace(statistic) / size_b + 1e-06
    shifted = statistic + ridge_term * identity
    scaling = jnp.sqrt(jnp.sum(shifted * shifted))
    current = shifted / scaling
    inverse = identity
    for step_number in range(ITERS):
        factor = (5.0 * identity - current) / 4.0
        if step_number == 0:
            inverse = scaling ** (-0.25) * factor
        else:
            inverse = jnp.dot(inverse, factor, precision=lax.Precision.HIGHEST)
        if step_number + 1 < ITERS:
            square = jnp.dot(factor, factor, precision=lax.Precision.HIGHEST)
            fourth = jnp.dot(square, square, precision=lax.Precision.HIGHEST)
            current = jnp.dot(fourth, current, precision=lax.Precision.HIGHEST)
    return inverse

def one_block(block_grads):
    widened = block_grads.astype(jnp.float32)
    left_sum = jnp.einsum('dij,dkj->ik', widened, widened, precision=lax.Precision.HIGHEST)
    right_sum = jnp.einsum('dji,djk->ik', widened, widened, precision=lax.Precision.HIGHEST)
    left_root = lax.optimization_barrier(inverse_root(left_sum).astype(jnp.bfloat16)).astype(jnp.float32)
    right_root = lax.optimization_barrier(inverse_root(right_sum).astype(jnp.bfloat16)).astype(jnp.float32)
    total_sum = lax.optimization_barrier(jnp.sum(widened, axis=0))
    middle = jnp.dot(left_root, total_sum, precision=lax.Precision.HIGHEST)
    return jnp.dot(middle, right_root, precision=lax.Precision.HIGHEST) / N_DP

def reference(gradients, block_layer):
    precond = lax.map(one_block, jnp.swapaxes(gradients, 0, 1))
    energy = lax.optimization_barrier(jnp.sum(precond * precond, axis=(1, 2)))
    selector = (block_layer[:, None] == jnp.arange(LAYERS, dtype=jnp.int32)[None, :]).astype(jnp.float32)
    layer_energy = lax.optimization_barrier(jnp.sum(selector * energy[:, None], axis=0))
    layer_count = lax.optimization_barrier(jnp.sum(selector, axis=0)) * float(B * B)
    block_mean = lax.optimization_barrier(jnp.sum(selector * layer_energy[None, :], axis=1)) / lax.optimization_barrier(jnp.sum(selector * layer_count[None, :], axis=1))
    return (precond * lax.rsqrt(block_mean + 1e-06)[:, None, None]).astype(jnp.bfloat16)
```

```python
import functools

import jax
import jax.numpy as jnp
from jax import lax
from jax.experimental import pallas as pl
from jax.experimental.pallas import tpu as pltpu
from jax.sharding import Mesh
from jax.sharding import PartitionSpec as P

LAYERS = 4
MESH_ID = pl.DeviceIdType.MESH
AXES = ("y", "z", "x", "h", "c")
NY, NZ, NX, NH, NC = 4, 8, 4, 2, 2
NP = NY * NZ
NT = NP // 2
B = 512
T = 128
NB = B // T
PAIRS = tuple((i, j) for i in range(NB) for j in range(i, NB))
PACKED = len(PAIRS) * T
CHUNK = PACKED // NT
COLS = B // NT
ROWS = B // NP
F32, BF16 = jnp.float32, jnp.bfloat16
DOT = functools.partial(lax.dot_general, preferred_element_type=F32)
NN = (((1,), (0,)), ((), ()))
NTR = (((1,), (1,)), ((), ()))


def split(x):
    high = x.astype(BF16)
    return high, (x - high.astype(F32)).astype(BF16)


def product(a, b):
    return DOT(a.astype(BF16), b.astype(BF16), NN)


def spread(j, size):
    return (size + size // 2 + ((j + 1) // 2) * (1 - 2 * (j % 2))) % size


def body(
    g_ref, layer_ref, out_ref,
    packed, rs_buf, ag_send, ag_buf, gt, gt_send, s_buf, stat, n0, n1, work, corr, root,
    t_send, t_buf, p_all, p_buf, ea_send, ea_buf, eb_send, eb_buf,
    rs_s, rs_r, ag_s, ag_r, sp_s, sp_r, t_s, t_r, p_s, p_r, ea_s, ea_r, eb_s, eb_r,
):
    y, z, x = lax.axis_index("y"), lax.axis_index("z"), lax.axis_index("x")
    h, c = lax.axis_index("h"), lax.axis_index("c")
    me = y * NZ + z
    team = (y + z) % 2
    member = y * (NZ // 2) + z // 2

    def at(**place):
        where = {"y": y, "z": z, "x": x, "h": h, "c": c}
        where.update(place)
        return tuple(where[name] for name in AXES)

    def send(src, dst, send_sem, recv_sem, where):
        pltpu.make_async_remote_copy(
            src_ref=src, dst_ref=dst, send_sem=send_sem, recv_sem=recv_sem,
            device_id=where, device_id_type=MESH_ID,
        ).start()

    def wait(ref, sem):
        pltpu.make_async_copy(ref, ref, sem).wait()

    barrier = pltpu.get_barrier_semaphore()

    def greet(where):
        pl.semaphore_signal(barrier, inc=1, device_id=where, device_id_type=MESH_ID)

    @pl.loop(0, NP - 1)
    def _(k):
        greet(at(y=(y + spread(k % NY, NY)) % NY, z=(z + spread(k // NY, NZ)) % NZ))

    @pl.loop(0, NY)
    def _(k):
        greet(at(y=k, h=1 - h, c=c))
        greet(at(y=k, h=h, c=1 - c))
        greet(at(y=k, h=1 - h, c=1 - c))

    @pl.loop(0, (NX - 1) * NZ)
    def _(k):
        greet(at(x=(x + 1 + k // NZ) % NX, z=k % NZ))

    g = g_ref[0, 0]
    gt_value = g.T
    gt[...] = gt_value.astype(F32)
    for which, m in ((0, g), (1, gt_value)):
        for half in range(2):
            lo = half * (B // 2)
            panel = DOT(m[lo : lo + B // 2], m[lo:], NTR)
            for n, (i, j) in enumerate(PAIRS):
                if i // (NB // 2) == half:
                    r, q = i * T - lo, j * T - lo
                    packed[which * PACKED + n * T : which * PACKED + (n + 1) * T, :] = panel[
                        r : r + T, q : q + T
                    ].astype(BF16)

    pl.semaphore_wait(barrier, NP - 1 + 3 * NY + (NX - 1) * NZ)

    @pl.loop(0, NP - 1)
    def _(k):
        yy, zz = (y + spread(k % NY, NY)) % NY, (z + spread(k // NY, NZ)) % NZ
        first = ((yy + zz) % 2) * PACKED + (yy * (NZ // 2) + zz // 2) * CHUNK
        send(
            packed.at[pl.ds(pl.multiple_of(first, 16), CHUNK), :], rs_buf.at[me], rs_s, rs_r, at(y=yy, z=zz)
        )

    mine = pl.multiple_of(team * PACKED + member * CHUNK, 16)
    rs_buf[me] = packed[pl.ds(mine, CHUNK), :]

    @pl.loop(0, NT)
    def _(m):
        parts = [gt[pl.ds(pl.multiple_of(T * q + 8 * m, 8), 8), :] for q in range(NB)]
        gt_send[m] = jnp.concatenate(parts, axis=0).astype(BF16)

    @pl.when(team == 0)
    def _():
        s_buf[me] = gt_send[member]

    wait(rs_buf.at[pl.ds(0, NP - 1)], rs_r)
    total = rs_buf[0].astype(F32)
    for k in range(1, NP):
        total = total + rs_buf[k].astype(F32)
    ag_send[...] = total.astype(BF16)
    ag_buf[pl.ds(pl.multiple_of(member * CHUNK, 16), CHUNK), :] = total.astype(BF16)

    def teammate(k, side):
        yy = (y + spread(k % NY, NY)) % NY
        half = (z // 2 + spread(k // NY, NZ // 2)) % (NZ // 2)
        return yy, 2 * half + (side + yy) % 2

    @pl.loop(0, NT - 1)
    def _(k):
        yy, zz = teammate(k, team)
        send(
            ag_send,
            ag_buf.at[pl.ds(pl.multiple_of(member * CHUNK, 16), CHUNK), :],
            ag_s, ag_r, at(y=yy, z=zz),
        )

    @pl.loop(0, NT - 1)
    def _(k):
        yy, zz = teammate(k, 0)
        send(gt_send.at[yy * (NZ // 2) + zz // 2], s_buf.at[me], sp_s, sp_r, at(y=yy, z=zz))

    @pl.when(team == 1)
    def _():
        yy, zz = teammate(NT - 1, 0)
        send(gt_send.at[yy * (NZ // 2) + zz // 2], s_buf.at[me], sp_s, sp_r, at(y=yy, z=zz))

    wait(ag_buf.at[pl.ds(0, (NT - 1) * CHUNK), :], ag_r)

    for n, (i, j) in enumerate(PAIRS):
        block = ag_buf[n * T : (n + 1) * T, :].astype(F32)
        stat[i * T : (i + 1) * T, j * T : (j + 1) * T] = block
        if i != j:
            stat[j * T : (j + 1) * T, i * T : (i + 1) * T] = block.T
    eye = lax.broadcasted_iota(jnp.int32, (B, B), 0) == lax.broadcasted_iota(jnp.int32, (B, B), 1)
    s = stat[...]
    trace = jnp.sum(jnp.where(eye, s, 0.0), axis=(0, 1), keepdims=True)
    ridge = 0.01 * trace / B + 1e-06
    a = s + jnp.where(eye, ridge, 0.0)
    square = jnp.sum(a * a, axis=(0, 1), keepdims=True)
    scale = lax.rsqrt(square)
    n0[...] = a * (0.2 * scale)
    work[...] = product(n0[...], n0[...]) - 2.0 * n0[...]
    work[...] = product(work[...], work[...]) + 2.0 * work[...]
    n1[...] = 1.25**4 * (product(work[...], n0[...]) + n0[...])
    corr[...] = product(n0[...], n1[...]) - n0[...] - n1[...]
    work[...] = product(n1[...], n1[...]) - 2.0 * n1[...]
    work[...] = product(work[...], work[...]) + 2.0 * work[...]
    n0[...] = 1.25**4 * (product(work[...], n1[...]) + n1[...])
    factor = 1.25**3 * lax.rsqrt(jnp.sqrt(jnp.sqrt(square)))
    inverse = corr[...] - n0[...] - product(corr[...], n0[...])
    root[...] = (factor * (inverse + jnp.where(eye, 1.0, 0.0))).astype(BF16)

    @pl.when(team == 0)
    def _():
        wait(s_buf.at[pl.ds(0, NP - 1)], sp_r)
        columns = s_buf[0].astype(F32)
        for k in range(1, NP):
            columns = columns + s_buf[k].astype(F32)
        high, low = split(columns)
        turned = DOT(high, root[...], NN) + DOT(low, root[...], NN)
        lane = lax.broadcasted_iota(jnp.int32, (8, T), 1) // COLS
        for e in range(NT):
            tile = jnp.zeros((8, T), F32)
            for q in range(NB):
                part = turned[8 * q : 8 * q + 8, T * (e // NB) : T * (e // NB) + T]
                shift = (COLS * (q - e % NB)) % T
                tile = jnp.where(lane == q, pltpu.roll(part, shift, 1) if shift else part, tile)
            t_send[8 * e : 8 * e + 8, :] = tile

        @pl.loop(0, NT)
        def _(k):
            yy, zz = teammate(k, 1)
            e = yy * (NZ // 2) + zz // 2
            send(
                t_send.at[pl.ds(pl.multiple_of(8 * e, 8), 8), :],
                t_buf.at[pl.ds(pl.multiple_of(8 * member, 8), 8), :],
                t_s, t_r, at(y=yy, z=zz),
            )

        ea_send[...] = jnp.zeros((1, T), F32)
        wait(p_buf, p_r)

    @pl.when(team == 1)
    def _():
        wait(t_buf, t_r)
        turned = t_buf[...].T
        rows = jnp.concatenate([turned[COLS * q : COLS * (q + 1), :] for q in range(NB)], axis=1)
        high, low = split(rows)
        p_all[...] = (DOT(high, root[...], NN) + DOT(low, root[...], NN)) / NP
        partner = z + 1 - 2 * (z % 2)
        send(
            p_all.at[pl.ds(pl.multiple_of(ROWS * (partner % 2), ROWS), ROWS), :],
            p_buf, p_s, p_r, at(z=partner),
        )
        lane = lax.broadcasted_iota(jnp.int32, (1, T), 1)
        energy = jnp.sum(p_all[...] * p_all[...], axis=(0, 1), keepdims=True)
        here = layer_ref[0]
        ea_send[...] = jnp.where(lane == here, energy, 0.0) + jnp.where(
            lane == here + LAYERS, float(COLS * B), 0.0
        )

    place = (y * NH + h) * NC + c
    ea_buf[place] = ea_send[...]

    @pl.loop(1, NY * NH * NC)
    def _(k):
        other = (place + k) % (NY * NH * NC)
        send(
            ea_send, ea_buf.at[place], ea_s, ea_r,
            at(y=other // (NH * NC), h=other // NC % NH, c=other % NC),
        )

    wait(ea_buf.at[pl.ds(0, NY * NH * NC - 1)], ea_r)
    eb_send[...] = jnp.sum(ea_buf[...], axis=0)
    spot = x * NZ + z
    eb_buf[spot] = eb_send[...]

    @pl.loop(1, NX * NZ)
    def _(k):
        other = (spot + k) % (NX * NZ)
        send(eb_send, eb_buf.at[spot], eb_s, eb_r, at(x=other // NZ, z=other % NZ))

    @pl.when(team == 1)
    def _():
        p_buf[...] = p_all[pl.ds(pl.multiple_of(ROWS * (z % 2), ROWS), ROWS), :]

    wait(eb_buf.at[pl.ds(0, NX * NZ - 1)], eb_r)
    sums = jnp.sum(eb_buf[...], axis=0)
    lane = lax.broadcasted_iota(jnp.int32, (1, T), 1)
    here = layer_ref[0]
    layer_square = jnp.sum(jnp.where(lane == here, sums, 0.0), axis=1, keepdims=True)
    layer_count = jnp.sum(jnp.where(lane == here + LAYERS, sums, 0.0), axis=1, keepdims=True)
    out_ref[0] = (p_buf[...] * lax.rsqrt(layer_square / layer_count + 1e-06)).astype(BF16)

    wait(rs_buf.at[pl.ds(0, NP - 1)], rs_s)
    wait(ag_buf.at[pl.ds(0, (NT - 1) * CHUNK), :], ag_s)
    wait(gt_send.at[pl.ds(0, NT - 1)], sp_s)
    wait(ea_buf.at[pl.ds(0, NY * NH * NC - 1)], ea_s)
    wait(eb_buf.at[pl.ds(0, NX * NZ - 1)], eb_s)

    @pl.when(team == 0)
    def _():
        wait(t_send, t_s)

    @pl.when(team == 1)
    def _():
        wait(gt_send.at[0], sp_s)
        wait(p_buf, p_s)


def per_device(gradients, block_layer):
    return pl.pallas_call(
        body,
        out_shape=jax.ShapeDtypeStruct((1, ROWS, B), BF16),
        in_specs=[
            pl.BlockSpec(memory_space=pltpu.VMEM),
            pl.BlockSpec(memory_space=pltpu.SMEM),
        ],
        out_specs=pl.BlockSpec(memory_space=pltpu.VMEM),
        scratch_shapes=[
            pltpu.VMEM((2 * PACKED, T), BF16),
            pltpu.VMEM((NP, CHUNK, T), BF16),
            pltpu.VMEM((CHUNK, T), BF16),
            pltpu.VMEM((PACKED, T), BF16),
            pltpu.VMEM((B, B), F32),
            pltpu.VMEM((NT, COLS, B), BF16),
            pltpu.VMEM((NP, COLS, B), BF16),
            pltpu.VMEM((B, B), F32),
            pltpu.VMEM((B, B), F32),
            pltpu.VMEM((B, B), F32),
            pltpu.VMEM((B, B), F32),
            pltpu.VMEM((B, B), F32),
            pltpu.VMEM((B, B), BF16),
            pltpu.VMEM((8 * NT, T), F32),
            pltpu.VMEM((8 * NT, T), F32),
            pltpu.VMEM((COLS, B), F32),
            pltpu.VMEM((ROWS, B), F32),
            pltpu.VMEM((1, T), F32),
            pltpu.VMEM((NY * NH * NC, 1, T), F32),
            pltpu.VMEM((1, T), F32),
            pltpu.VMEM((NX * NZ, 1, T), F32),
        ]
        + [pltpu.SemaphoreType.DMA] * 14,
        compiler_params=pltpu.CompilerParams(
            collective_id=0, has_side_effects=True, vmem_limit_bytes=60 * 1024 * 1024
        ),
    )(gradients, block_layer)


def solution(mesh):
    finer = Mesh(mesh.devices.reshape(NY, NZ, NX, NH, NC), AXES)
    return jax.shard_map(
        per_device,
        mesh=finer,
        in_specs=(P(("y", "z"), ("x", "h", "c"), None, None), P(("x", "h", "c"))),
        out_specs=P(("x", "h", "c"), ("y", "z"), None),
        check_vma=False,
    )
```

```python
import functools

import jax
import jax.numpy as jnp
from jax import lax
from jax.experimental import pallas as pl
from jax.experimental.pallas import tpu as pltpu
from jax.sharding import Mesh
from jax.sharding import PartitionSpec as P

LAYERS = 4
MESH_ID = pl.DeviceIdType.MESH
AXES = ("y", "z", "x", "h", "c")
NY, NZ, NX, NH, NC = 4, 8, 4, 2, 2
NP = NY * NZ
NT = NP // 2
B = 512
T = 128
NB = B // T
HALF = T // 2
PACKED = NB * (NB - 1) // 2 * T + NB * HALF + NB // 2 * HALF
CHUNK = PACKED // NT
VIA_Z = 32
VIA_Y = CHUNK - VIA_Z
COLS = B // NT
ROWS = B // NP
F32, BF16 = jnp.float32, jnp.bfloat16
DOT = functools.partial(lax.dot_general, preferred_element_type=F32)
NN = (((1,), (0,)), ((), ()))
NTR = (((1,), (1,)), ((), ()))


def split(x):
    high = x.astype(BF16)
    return high, (x - high.astype(F32)).astype(BF16)


def product(a, b):
    return DOT(a.astype(BF16), b.astype(BF16), NN)


def spread(j, size):
    return (size + size // 2 + ((j + 1) // 2) * (1 - 2 * (j % 2))) % size


def body(
    g_hbm, layer_ref, out_ref,
    g_ref, gt, packed, z_pack, y_pack, z_buf, y_buf, z_mid, y_mid, z_end, y_end,
    ag_send, ag_buf, zs_pack, ys_pack, zs_buf, ys_buf, zs_mid, ys_mid, zs_end, ys_end,
    stat, n0, n1, work, corr, root,
    t_send, t_buf, p_all, p_buf, ea_send, ea_buf, eb_send, eb_buf, sems,
):
    y, z, x = lax.axis_index("y"), lax.axis_index("z"), lax.axis_index("x")
    h, c = lax.axis_index("h"), lax.axis_index("c")
    team = (y + z) % 2
    member = y * (NZ // 2) + z // 2
    (g_sem, z1s, z1r, y1s, y1r, z2s, z2r, y2s, y2r, ags, agr, zs1s, zs1r, ys1s, ys1r,
     zs2s, zs2r, ys2s, ys2r, ts, tr, ps, pr, eas, ear, ebs, ebr) = [sems.at[k] for k in range(27)]

    def at(**place):
        where = {"y": y, "z": z, "x": x, "h": h, "c": c}
        where.update(place)
        return tuple(where[name] for name in AXES)

    def send(src, dst, send_sem, recv_sem, where):
        pltpu.make_async_remote_copy(
            src_ref=src, dst_ref=dst, send_sem=send_sem, recv_sem=recv_sem,
            device_id=where, device_id_type=MESH_ID,
        ).start()

    def wait(ref, sem):
        pltpu.make_async_copy(ref, ref, sem).wait()

    load = pltpu.make_async_copy(g_hbm.at[0, 0], g_ref, g_sem)
    load.start()

    barrier = pltpu.get_barrier_semaphore()

    def greet(where):
        pl.semaphore_signal(barrier, inc=1, device_id=where, device_id_type=MESH_ID)

    @pl.loop(0, NP - 1)
    def _(k):
        greet(at(y=(y + spread(k % NY, NY)) % NY, z=(z + spread(k // NY, NZ)) % NZ))

    @pl.loop(0, (NX - 1) * NZ)
    def _(k):
        greet(at(x=(x + 1 + k // NZ) % NX, z=(z + spread(k % NZ, NZ)) % NZ))

    @pl.loop(0, NY)
    def _(k):
        greet(at(y=k, h=1 - h, c=c))
        greet(at(y=k, h=h, c=1 - c))
        greet(at(y=k, h=1 - h, c=1 - c))

    load.wait()
    g = g_ref[...]
    gt_value = g.T
    gt[...] = gt_value.astype(F32)
    for side, m in ((0, g), (1, gt_value)):
        row = 0
        corners = []
        for half in range(2):
            lo = half * (B // 2)
            panel = DOT(m[lo : lo + B // 2], m[lo:], NTR)
            for i in range(half * NB // 2, (half + 1) * NB // 2):
                for j in range(i, NB):
                    r, q = i * T - lo, j * T - lo
                    size = HALF if i == j else T
                    packed[side, row : row + size, :] = panel[r : r + size, q : q + T]
                    row += size
                    if i == j:
                        corners.append(panel[r + HALF : r + T, q : q + T])
        lane = lax.broadcasted_iota(jnp.int32, (HALF, T), 1)
        for k in range(0, NB, 2):
            packed[side, row : row + HALF, :] = jnp.where(
                lane < HALF, pltpu.roll(corners[k], HALF, 1), corners[k + 1]
            )
            row += HALF
    for yy in range(NY):
        for zz in range(NZ):
            side, first = (yy + zz) % 2, (yy * (NZ // 2) + zz // 2) * CHUNK
            z_pack[zz, yy] = packed[side, first : first + VIA_Z, :].astype(BF16)
            y_pack[yy, zz] = packed[side, first + VIA_Z : first + CHUNK, :].astype(BF16)

    pl.semaphore_wait(barrier, NP - 1 + 3 * NY + (NX - 1) * NZ)

    def along_y(source, target, send_sem, recv_sem):
        @pl.loop(0, NY - 1)
        def _(k):
            yy = (y + spread(k, NY)) % NY
            send(source.at[yy], target.at[y], send_sem, recv_sem, at(y=yy))

    def along_z(source, target, send_sem, recv_sem):
        @pl.loop(0, NZ - 1)
        def _(k):
            zz = (z + spread(k, NZ)) % NZ
            send(source.at[zz], target.at[z], send_sem, recv_sem, at(z=zz))

    def total(ref, count):
        result = ref[0].astype(F32)
        for k in range(1, count):
            result = result + ref[k].astype(F32)
        return result

    along_y(y_pack, y_buf, y1s, y1r)
    along_z(z_pack, z_buf, z1s, z1r)
    y_buf[y] = y_pack[y]
    z_buf[z] = z_pack[z]

    def columns(m, first):
        parts = [gt[T * q + 8 * m : T * q + 8 * m + 8, :] for q in range(first, first + NB // 2)]
        return jnp.concatenate(parts, axis=0).astype(BF16)

    for zz in range(NZ):
        for k in range(NY // 2):
            zs_pack[zz, k] = columns((zz % 2 + 2 * k) * (NZ // 2) + zz // 2, 0)
    for yy in range(NY):
        for k in range(NZ // 2):
            ys_pack[yy, k] = columns(yy * (NZ // 2) + k, NB // 2)
    ys_buf[y] = ys_pack[y]
    zs_buf[z] = zs_pack[z]

    wait(z_buf.at[pl.ds(0, NZ - 1)], z1r)
    z_mid[...] = total(z_buf, NZ).astype(BF16)
    along_y(z_mid, z_end, z2s, z2r)
    z_end[y] = z_mid[y]
    wait(y_buf.at[pl.ds(0, NY - 1)], y1r)
    y_mid[...] = total(y_buf, NY).astype(BF16)
    along_z(y_mid, y_end, y2s, y2r)
    y_end[z] = y_mid[z]
    along_y(ys_pack, ys_buf, ys1s, ys1r)
    along_z(zs_pack, zs_buf, zs1s, zs1r)

    wait(z_end.at[pl.ds(0, NY - 1)], z2r)
    wait(y_end.at[pl.ds(0, NZ - 1)], y2r)
    mine = jnp.concatenate([total(z_end, NY), total(y_end, NZ)], axis=0).astype(BF16)
    ag_send[...] = mine
    ag_buf[member] = mine

    def teammate(k, side):
        yy = (y + spread(k % NY, NY)) % NY
        half = (z // 2 + spread(k // NY, NZ // 2)) % (NZ // 2)
        return yy, 2 * half + (side + yy) % 2

    @pl.loop(0, NT - 1)
    def _(k):
        yy, zz = teammate(k, team)
        send(ag_send, ag_buf.at[member], ags, agr, at(y=yy, z=zz))

    wait(zs_buf.at[pl.ds(0, NZ - 1)], zs1r)
    zs_mid[...] = total(zs_buf, NZ)
    for k in range(NY // 2):
        yy = z % 2 + 2 * k

        @pl.when(yy != y)
        def _(k=k, yy=yy):
            send(zs_mid.at[k], zs_end.at[y], zs2s, zs2r, at(y=yy))

    wait(ys_buf.at[pl.ds(0, NY - 1)], ys1r)
    ys_mid[...] = total(ys_buf, NY)
    for k in range(NZ // 2):
        zz = y % 2 + 2 * k

        @pl.when(zz != z)
        def _(k=k, zz=zz):
            send(ys_mid.at[k], ys_end.at[z], ys2s, ys2r, at(z=zz))

    wait(ag_buf.at[pl.ds(0, NT - 1)], agr)

    whole = jnp.concatenate([ag_buf[k].astype(F32) for k in range(NT)], axis=0)
    row = 0
    spare = PACKED - NB // 2 * HALF
    lower = lax.broadcasted_iota(jnp.int32, (T, T), 0) >= HALF
    left = lax.broadcasted_iota(jnp.int32, (T, T), 1) < HALF
    for i in range(NB):
        for j in range(i, NB):
            if i == j:
                corner = whole[spare + i // 2 * HALF : spare + (i // 2 + 1) * HALF]
                corner = corner if i % 2 else pltpu.roll(corner, HALF, 1)
                block = jnp.concatenate([whole[row : row + HALF], corner], axis=0)
                block = jnp.where(lower & left, block.T, block)
                row += HALF
            else:
                block = whole[row : row + T]
                stat[j * T : (j + 1) * T, i * T : (i + 1) * T] = block.T
                row += T
            stat[i * T : (i + 1) * T, j * T : (j + 1) * T] = block
    eye = lax.broadcasted_iota(jnp.int32, (B, B), 0) == lax.broadcasted_iota(jnp.int32, (B, B), 1)
    s = stat[...]
    trace = jnp.sum(jnp.where(eye, s, 0.0), axis=(0, 1), keepdims=True)
    ridge = 0.01 * trace / B + 1e-06
    a = s + jnp.where(eye, ridge, 0.0)
    square = jnp.sum(a * a, axis=(0, 1), keepdims=True)
    scale = lax.rsqrt(square)
    n0[...] = a * (0.2 * scale)
    work[...] = product(n0[...], n0[...]) - 2.0 * n0[...]
    work[...] = product(work[...], work[...]) + 2.0 * work[...]
    n1[...] = 1.25**4 * (product(work[...], n0[...]) + n0[...])
    corr[...] = product(n0[...], n1[...]) - n0[...] - n1[...]
    work[...] = product(n1[...], n1[...]) - 2.0 * n1[...]
    work[...] = product(work[...], work[...]) + 2.0 * work[...]
    n0[...] = 1.25**4 * (product(work[...], n1[...]) + n1[...])
    factor = 1.25**3 * lax.rsqrt(jnp.sqrt(jnp.sqrt(square)))
    inverse = corr[...] - n0[...] - product(corr[...], n0[...])
    root[...] = (factor * (inverse + jnp.where(eye, 1.0, 0.0))).astype(BF16)

    @pl.when(team == 0)
    def _():
        wait(zs_end.at[pl.ds(0, NY - 1)], zs2r)
        wait(ys_end.at[pl.ds(0, NZ - 1)], ys2r)
        zs_end[y] = zs_mid[y // 2]
        ys_end[z] = ys_mid[z // 2]
        summed = jnp.concatenate([total(zs_end, NY), total(ys_end, NZ)], axis=0)
        high, low = split(summed)
        turned = DOT(high, root[...], NN) + DOT(low, root[...], NN)
        lane = lax.broadcasted_iota(jnp.int32, (8, T), 1) // COLS
        for e in range(NT):
            tile = jnp.zeros((8, T), F32)
            for q in range(NB):
                part = turned[8 * q : 8 * q + 8, T * (e // NB) : T * (e // NB) + T]
                shift = (COLS * (q - e % NB)) % T
                tile = jnp.where(lane == q, pltpu.roll(part, shift, 1) if shift else part, tile)
            t_send[8 * e : 8 * e + 8, :] = tile

        @pl.loop(0, NT)
        def _(k):
            yy, zz = teammate(k, 1)
            e = yy * (NZ // 2) + zz // 2
            send(
                t_send.at[pl.ds(pl.multiple_of(8 * e, 8), 8), :],
                t_buf.at[pl.ds(pl.multiple_of(8 * member, 8), 8), :],
                ts, tr, at(y=yy, z=zz),
            )

        ea_send[...] = jnp.zeros((1, T), F32)

    @pl.when(team == 1)
    def _():
        wait(t_buf, tr)

    @pl.when(team == 1)
    def _():
        turned = t_buf[...].T
        rows = jnp.concatenate([turned[COLS * q : COLS * (q + 1), :] for q in range(NB)], axis=1)
        high, low = split(rows)
        p_all[...] = (DOT(high, root[...], NN) + DOT(low, root[...], NN)) / NP
        lane = lax.broadcasted_iota(jnp.int32, (1, T), 1)
        energy = jnp.sum(p_all[...] * p_all[...], axis=(0, 1), keepdims=True)
        here = layer_ref[0]
        ea_send[...] = jnp.where(lane == here, energy, 0.0) + jnp.where(
            lane == here + LAYERS, float(COLS * B), 0.0
        )

    place = (y * NH + h) * NC + c
    ea_buf[place] = ea_send[...]

    @pl.loop(1, NY * NH * NC)
    def _(k):
        other = (place + k) % (NY * NH * NC)
        send(
            ea_send, ea_buf.at[place], eas, ear,
            at(y=other // (NH * NC), h=other // NC % NH, c=other % NC),
        )

    @pl.when(team == 1)
    def _():
        partner = z + 1 - 2 * (z % 2)
        send(
            p_all.at[pl.ds(pl.multiple_of(ROWS * (partner % 2), ROWS), ROWS), :],
            p_buf, ps, pr, at(z=partner),
        )
        p_buf[...] = p_all[pl.ds(pl.multiple_of(ROWS * (z % 2), ROWS), ROWS), :]

    wait(ea_buf.at[pl.ds(0, NY * NH * NC - 1)], ear)
    eb_send[...] = jnp.sum(ea_buf[...], axis=0)
    spot = x * NZ + z
    eb_buf[spot] = eb_send[...]

    @pl.loop(0, NX * NZ - 1)
    def _(k):
        xx = (x + spread(k % NX, NX)) % NX
        zz = (z + spread(k // NX, NZ)) % NZ
        send(eb_send, eb_buf.at[spot], ebs, ebr, at(x=xx, z=zz))

    @pl.when(team == 0)
    def _():
        wait(p_buf, pr)

    wait(eb_buf.at[pl.ds(0, NX * NZ - 1)], ebr)
    sums = jnp.sum(eb_buf[...], axis=0)
    lane = lax.broadcasted_iota(jnp.int32, (1, T), 1)
    here = layer_ref[0]
    layer_square = jnp.sum(jnp.where(lane == here, sums, 0.0), axis=1, keepdims=True)
    layer_count = jnp.sum(jnp.where(lane == here + LAYERS, sums, 0.0), axis=1, keepdims=True)
    out_ref[0] = (p_buf[...] * lax.rsqrt(layer_square / layer_count + 1e-06)).astype(BF16)

    for ref, count, sem in (
        (y_buf, NY, y1s), (z_buf, NZ, z1s), (z_end, NY, z2s), (y_end, NZ, y2s), (ag_buf, NT, ags),
        (ys_buf, NY, ys1s), (zs_buf, NZ, zs1s), (ea_buf, NY * NH * NC, eas), (eb_buf, NX * NZ, ebs),
    ):
        wait(ref.at[pl.ds(0, count - 1)], sem)
    wait(zs_mid.at[pl.ds(0, NY // 2 - 1)], zs2s)
    wait(ys_mid.at[pl.ds(0, NZ // 2 - 1)], ys2s)

    @pl.when(team == 0)
    def _():
        wait(t_send, ts)

    @pl.when(team == 1)
    def _():
        wait(zs_mid.at[0], zs2s)
        wait(ys_mid.at[0], ys2s)
        wait(p_buf, ps)


def per_device(gradients, block_layer):
    return pl.pallas_call(
        body,
        out_shape=jax.ShapeDtypeStruct((1, ROWS, B), BF16),
        in_specs=[
            pl.BlockSpec(memory_space=pl.ANY),
            pl.BlockSpec(memory_space=pltpu.SMEM),
        ],
        out_specs=pl.BlockSpec(memory_space=pltpu.VMEM),
        scratch_shapes=[
            pltpu.VMEM((B, B), BF16),
            pltpu.VMEM((B, B), F32),
            pltpu.VMEM((2, PACKED, T), F32),
            pltpu.VMEM((NZ, NY, VIA_Z, T), BF16),
            pltpu.VMEM((NY, NZ, VIA_Y, T), BF16),
            pltpu.VMEM((NZ, NY, VIA_Z, T), BF16),
            pltpu.VMEM((NY, NZ, VIA_Y, T), BF16),
            pltpu.VMEM((NY, VIA_Z, T), BF16),
            pltpu.VMEM((NZ, VIA_Y, T), BF16),
            pltpu.VMEM((NY, VIA_Z, T), BF16),
            pltpu.VMEM((NZ, VIA_Y, T), BF16),
            pltpu.VMEM((CHUNK, T), BF16),
            pltpu.VMEM((NT, CHUNK, T), BF16),
            pltpu.VMEM((NZ, NY // 2, COLS // 2, B), BF16),
            pltpu.VMEM((NY, NZ // 2, COLS // 2, B), BF16),
            pltpu.VMEM((NZ, NY // 2, COLS // 2, B), BF16),
            pltpu.VMEM((NY, NZ // 2, COLS // 2, B), BF16),
            pltpu.VMEM((NY // 2, COLS // 2, B), F32),
            pltpu.VMEM((NZ // 2, COLS // 2, B), F32),
            pltpu.VMEM((NY, COLS // 2, B), F32),
            pltpu.VMEM((NZ, COLS // 2, B), F32),
        ]
        + [pltpu.VMEM((B, B), F32)] * 5
        + [
            pltpu.VMEM((B, B), BF16),
            pltpu.VMEM((8 * NT, T), F32),
            pltpu.VMEM((8 * NT, T), F32),
            pltpu.VMEM((COLS, B), F32),
            pltpu.VMEM((ROWS, B), F32),
            pltpu.VMEM((1, T), F32),
            pltpu.VMEM((NY * NH * NC, 1, T), F32),
            pltpu.VMEM((1, T), F32),
            pltpu.VMEM((NX * NZ, 1, T), F32),
            pltpu.SemaphoreType.DMA((27,)),
        ],
        compiler_params=pltpu.CompilerParams(
            collective_id=0, has_side_effects=True, vmem_limit_bytes=60 * 1024 * 1024
        ),
    )(gradients, block_layer)


def solution(mesh):
    finer = Mesh(mesh.devices.reshape(NY, NZ, NX, NH, NC), AXES)
    return jax.shard_map(
        per_device,
        mesh=finer,
        in_specs=(P(("y", "z"), ("x", "h", "c"), None, None), P(("x", "h", "c"))),
        out_specs=P(("x", "h", "c"), ("y", "z"), None),
        check_vma=False,
    )
```

```python
import functools

import jax
import jax.numpy as jnp
from jax import lax
from jax.experimental import pallas as pl
from jax.experimental.pallas import tpu as pltpu
from jax.sharding import Mesh
from jax.sharding import PartitionSpec as P

LAYERS = 4
MESH_ID = pl.DeviceIdType.MESH
AXES = ("y", "z", "x", "h", "c")
NY, NZ, NX, NH, NC = 4, 8, 4, 2, 2
NP = NY * NZ
NT = NP // 2
B = 512
T = 128
NB = B // T
HALF = T // 2
PACKED = NB * (NB - 1) // 2 * T + NB * HALF + NB // 2 * HALF
CHUNK = PACKED // NT
VIA_Z = 32
VIA_Y = CHUNK - VIA_Z
COLS = B // NT
ROWS = B // NP
F32, BF16 = jnp.float32, jnp.bfloat16
DOT = functools.partial(lax.dot_general, preferred_element_type=F32)
NN = (((1,), (0,)), ((), ()))
NTR = (((1,), (1,)), ((), ()))


def split(x):
    high = x.astype(BF16)
    return high, (x - high.astype(F32)).astype(BF16)


def product(a, b):
    return DOT(a.astype(BF16), b.astype(BF16), NN)


def spread(size):
    return sorted(range(size), key=lambda d: -min(d, size - d))


def pairs_of(first, second):
    far = [(a, b) for a in spread(first) for b in spread(second)]
    return sorted(far, key=lambda p: -min(p[0], first - p[0]) - min(p[1], second - p[1]))


def body(
    g_hbm, layer_hbm, out_ref,
    g_ref, gt, packed, z_pack, y_pack, z_buf, y_buf, z_mid, y_mid, z_end, y_end,
    ag_send, ag_buf, zs_pack, ys_pack, zs_buf, ys_buf, zs_mid, ys_mid, zs_end, ys_end,
    stat, n0, n1, work, corr, root,
    t_send, t_buf, p_all, p_buf, ea_send, ea_buf, eb_send, eb_buf, layer_ref, sems,
):
    y, z, x = lax.axis_index("y"), lax.axis_index("z"), lax.axis_index("x")
    h, c = lax.axis_index("h"), lax.axis_index("c")
    team = (y + z) % 2
    member = y * (NZ // 2) + lax.div(z, 2)
    ys = [lax.rem(y + d, NY) for d in range(NY)]
    zs = [lax.rem(z + d, NZ) for d in range(NZ)]
    xs = [lax.rem(x + d, NX) for d in range(NX)]
    halves = [lax.rem(lax.div(z, 2) + d, NZ // 2) for d in range(NZ // 2)]
    (g_sem, z1s, z1r, y1s, y1r, z2s, z2r, y2s, y2r, ags, agr, zs1s, zs1r, ys1s, ys1r,
     zs2s, zs2r, ys2s, ys2r, ts, tr, ps, pr, eas, ear, ebs, ebr) = [sems.at[k] for k in range(27)]
    layer_sem = sems.at[27]

    def at(**place):
        where = {"y": y, "z": z, "x": x, "h": h, "c": c}
        where.update(place)
        return tuple(where[name] for name in AXES)

    def send(src, dst, send_sem, recv_sem, where):
        pltpu.make_async_remote_copy(
            src_ref=src, dst_ref=dst, send_sem=send_sem, recv_sem=recv_sem,
            device_id=where, device_id_type=MESH_ID,
        ).start()

    def wait(ref, sem):
        pltpu.make_async_copy(ref, ref, sem).wait()

    load = pltpu.make_async_copy(g_hbm.at[0, 0], g_ref, g_sem)
    load.start()
    load_layer = pltpu.make_async_copy(layer_hbm, layer_ref, layer_sem)
    load_layer.start()

    barrier = pltpu.get_barrier_semaphore()

    def greet(where):
        pl.semaphore_signal(barrier, inc=1, device_id=where, device_id_type=MESH_ID)

    for dx, dz in pairs_of(NX, NZ):
        if dx:
            greet(at(x=xs[dx], z=zs[dz]))
    for dy in spread(NY):
        greet(at(y=ys[dy], h=1 - h, c=c))
        greet(at(y=ys[dy], h=h, c=1 - c))
        greet(at(y=ys[dy], h=1 - h, c=1 - c))
    for dy, dz in pairs_of(NY, NZ)[:-1]:
        greet(at(y=ys[dy], z=zs[dz]))

    load.wait()
    load_layer.wait()
    g = g_ref[...]
    gt_value = g.T
    gt[...] = gt_value.astype(F32)
    for side, m in ((0, g), (1, gt_value)):
        row = 0
        corners = []
        for half in range(2):
            lo = half * (B // 2)
            panel = DOT(m[lo : lo + B // 2], m[lo:], NTR)
            for i in range(half * NB // 2, (half + 1) * NB // 2):
                for j in range(i, NB):
                    r, q = i * T - lo, j * T - lo
                    size = HALF if i == j else T
                    packed[side, row : row + size, :] = panel[r : r + size, q : q + T]
                    row += size
                    if i == j:
                        corners.append(panel[r + HALF : r + T, q : q + T])
        lane = lax.broadcasted_iota(jnp.int32, (HALF, T), 1)
        for k in range(0, NB, 2):
            packed[side, row : row + HALF, :] = jnp.where(
                lane < HALF, pltpu.roll(corners[k], HALF, 1), corners[k + 1]
            )
            row += HALF
    for yy in range(NY):
        for zz in range(NZ):
            side, first = (yy + zz) % 2, (yy * (NZ // 2) + zz // 2) * CHUNK
            z_pack[zz, yy] = packed[side, first : first + VIA_Z, :].astype(BF16)
            y_pack[yy, zz] = packed[side, first + VIA_Z : first + CHUNK, :].astype(BF16)

    pl.semaphore_wait(barrier, NP - 1 + 3 * NY + (NX - 1) * NZ)

    def along_y(source, target, send_sem, recv_sem):
        for d in spread(NY)[:-1]:
            send(source.at[ys[d]], target.at[y], send_sem, recv_sem, at(y=ys[d]))

    def along_z(source, target, send_sem, recv_sem):
        for d in spread(NZ)[:-1]:
            send(source.at[zs[d]], target.at[z], send_sem, recv_sem, at(z=zs[d]))

    def total(ref, count):
        result = ref[0].astype(F32)
        for k in range(1, count):
            result = result + ref[k].astype(F32)
        return result

    along_y(y_pack, y_buf, y1s, y1r)
    along_z(z_pack, z_buf, z1s, z1r)
    y_buf[y] = y_pack[y]
    z_buf[z] = z_pack[z]

    def columns(m, first):
        parts = [gt[T * q + 8 * m : T * q + 8 * m + 8, :] for q in range(first, first + NB // 2)]
        return jnp.concatenate(parts, axis=0).astype(BF16)

    for zz in range(NZ):
        for k in range(NY // 2):
            zs_pack[zz, k] = columns((zz % 2 + 2 * k) * (NZ // 2) + zz // 2, 0)
    for yy in range(NY):
        for k in range(NZ // 2):
            ys_pack[yy, k] = columns(yy * (NZ // 2) + k, NB // 2)
    ys_buf[y] = ys_pack[y]
    zs_buf[z] = zs_pack[z]

    along_y(ys_pack, ys_buf, ys1s, ys1r)
    along_z(zs_pack, zs_buf, zs1s, zs1r)

    wait(z_buf.at[pl.ds(0, NZ - 1)], z1r)
    z_mid[...] = total(z_buf, NZ).astype(BF16)
    along_y(z_mid, z_end, z2s, z2r)
    z_end[y] = z_mid[y]
    wait(y_buf.at[pl.ds(0, NY - 1)], y1r)
    y_mid[...] = total(y_buf, NY).astype(BF16)
    along_z(y_mid, y_end, y2s, y2r)
    y_end[z] = y_mid[z]
    wait(z_end.at[pl.ds(0, NY - 1)], z2r)
    wait(y_end.at[pl.ds(0, NZ - 1)], y2r)
    mine = jnp.concatenate([total(z_end, NY), total(y_end, NZ)], axis=0).astype(BF16)
    ag_send[...] = mine
    ag_buf[member] = mine

    for dy, dh in pairs_of(NY, NZ // 2)[:-1]:
        zz = 2 * halves[dh] + lax.rem(team + ys[dy], 2)
        send(ag_send, ag_buf.at[member], ags, agr, at(y=ys[dy], z=zz))

    wait(zs_buf.at[pl.ds(0, NZ - 1)], zs1r)
    zs_mid[...] = total(zs_buf, NZ)
    for k in range(NY // 2):
        yy = z % 2 + 2 * k

        @pl.when(yy != y)
        def _(k=k, yy=yy):
            send(zs_mid.at[k], zs_end.at[y], zs2s, zs2r, at(y=yy))

    wait(ys_buf.at[pl.ds(0, NY - 1)], ys1r)
    ys_mid[...] = total(ys_buf, NY)
    for k in range(NZ // 2):
        zz = y % 2 + 2 * k

        @pl.when(zz != z)
        def _(k=k, zz=zz):
            send(ys_mid.at[k], ys_end.at[z], ys2s, ys2r, at(z=zz))

    wait(ag_buf.at[pl.ds(0, NT - 1)], agr)

    whole = jnp.concatenate([ag_buf[k].astype(F32) for k in range(NT)], axis=0)
    row = 0
    spare = PACKED - NB // 2 * HALF
    lower = lax.broadcasted_iota(jnp.int32, (T, T), 0) >= HALF
    left = lax.broadcasted_iota(jnp.int32, (T, T), 1) < HALF
    for i in range(NB):
        for j in range(i, NB):
            if i == j:
                corner = whole[spare + i // 2 * HALF : spare + (i // 2 + 1) * HALF]
                corner = corner if i % 2 else pltpu.roll(corner, HALF, 1)
                block = jnp.concatenate([whole[row : row + HALF], corner], axis=0)
                block = jnp.where(lower & left, block.T, block)
                row += HALF
            else:
                block = whole[row : row + T]
                stat[j * T : (j + 1) * T, i * T : (i + 1) * T] = block.T
                row += T
            stat[i * T : (i + 1) * T, j * T : (j + 1) * T] = block
    eye = lax.broadcasted_iota(jnp.int32, (B, B), 0) == lax.broadcasted_iota(jnp.int32, (B, B), 1)
    s = stat[...]
    trace = jnp.sum(jnp.where(eye, s, 0.0), axis=(0, 1), keepdims=True)
    ridge = 0.01 * trace / B + 1e-06
    a = s + jnp.where(eye, ridge, 0.0)
    square = jnp.sum(a * a, axis=(0, 1), keepdims=True)
    scale = lax.rsqrt(square)
    n0[...] = a * (0.2 * scale)
    work[...] = product(n0[...], n0[...]) - 2.0 * n0[...]
    work[...] = product(work[...], work[...]) + 2.0 * work[...]
    n1[...] = 1.25**4 * (product(work[...], n0[...]) + n0[...])
    corr[...] = product(n0[...], n1[...]) - n0[...] - n1[...]
    work[...] = product(n1[...], n1[...]) - 2.0 * n1[...]
    work[...] = product(work[...], work[...]) + 2.0 * work[...]
    n0[...] = 1.25**4 * (product(work[...], n1[...]) + n1[...])
    factor = 1.25**3 * lax.rsqrt(jnp.sqrt(jnp.sqrt(square)))
    inverse = corr[...] - n0[...] - product(corr[...], n0[...])
    root[...] = (factor * (inverse + jnp.where(eye, 1.0, 0.0))).astype(BF16)

    @pl.when(team == 0)
    def _():
        wait(zs_end.at[pl.ds(0, NY - 1)], zs2r)
        wait(ys_end.at[pl.ds(0, NZ - 1)], ys2r)
        zs_end[y] = zs_mid[y // 2]
        ys_end[z] = ys_mid[z // 2]
        summed = jnp.concatenate([total(zs_end, NY), total(ys_end, NZ)], axis=0)
        high, low = split(summed)
        turned = DOT(high, root[...], NN) + DOT(low, root[...], NN)
        lane = lax.broadcasted_iota(jnp.int32, (8, T), 1) // COLS
        for e in range(NT):
            tile = jnp.zeros((8, T), F32)
            for q in range(NB):
                part = turned[8 * q : 8 * q + 8, T * (e // NB) : T * (e // NB) + T]
                shift = (COLS * (q - e % NB)) % T
                tile = jnp.where(lane == q, pltpu.roll(part, shift, 1) if shift else part, tile)
            t_send[8 * e : 8 * e + 8, :] = tile

        for dy, dh in pairs_of(NY, NZ // 2):
            e = ys[dy] * (NZ // 2) + halves[dh]
            send(
                t_send.at[pl.ds(pl.multiple_of(8 * e, 8), 8), :],
                t_buf.at[pl.ds(pl.multiple_of(8 * member, 8), 8), :],
                ts, tr, at(y=ys[dy], z=2 * halves[dh] + lax.rem(1 + ys[dy], 2)),
            )

        ea_send[...] = jnp.zeros((1, T), F32)

    @pl.when(team == 1)
    def _():
        wait(t_buf, tr)

    @pl.when(team == 1)
    def _():
        turned = t_buf[...].T
        rows = jnp.concatenate([turned[COLS * q : COLS * (q + 1), :] for q in range(NB)], axis=1)
        high, low = split(rows)
        p_all[...] = (DOT(high, root[...], NN) + DOT(low, root[...], NN)) / NP
        lane = lax.broadcasted_iota(jnp.int32, (1, T), 1)
        energy = jnp.sum(p_all[...] * p_all[...], axis=(0, 1), keepdims=True)
        here = layer_ref[0]
        ea_send[...] = jnp.where(lane == here, energy, 0.0) + jnp.where(
            lane == here + LAYERS, float(COLS * B), 0.0
        )

    place = (y * NH + h) * NC + c
    ea_buf[place] = ea_send[...]

    for hh in (1 - h, h):
        for dy in spread(NY):
            for cc in (1 - c, c):
                if not (hh is h and cc is c and dy == 0):
                    send(ea_send, ea_buf.at[place], eas, ear, at(y=ys[dy], h=hh, c=cc))

    @pl.when(team == 1)
    def _():
        partner = z + 1 - 2 * (z % 2)
        send(
            p_all.at[pl.ds(pl.multiple_of(ROWS * (partner % 2), ROWS), ROWS), :],
            p_buf, ps, pr, at(z=partner),
        )
        p_buf[...] = p_all[pl.ds(pl.multiple_of(ROWS * (z % 2), ROWS), ROWS), :]

    wait(ea_buf.at[pl.ds(0, NY * NH * NC - 1)], ear)
    eb_send[...] = jnp.sum(ea_buf[...], axis=0)
    spot = x * NZ + z
    eb_buf[spot] = eb_send[...]

    for dx, dz in pairs_of(NX, NZ)[:-1]:
        send(eb_send, eb_buf.at[spot], ebs, ebr, at(x=xs[dx], z=zs[dz]))

    @pl.when(team == 0)
    def _():
        wait(p_buf, pr)

    wait(eb_buf.at[pl.ds(0, NX * NZ - 1)], ebr)
    sums = jnp.sum(eb_buf[...], axis=0)
    lane = lax.broadcasted_iota(jnp.int32, (1, T), 1)
    here = layer_ref[0]
    layer_square = jnp.sum(jnp.where(lane == here, sums, 0.0), axis=1, keepdims=True)
    layer_count = jnp.sum(jnp.where(lane == here + LAYERS, sums, 0.0), axis=1, keepdims=True)
    out_ref[0] = (p_buf[...] * lax.rsqrt(layer_square / layer_count + 1e-06)).astype(BF16)

    for ref, count, sem in (
        (y_buf, NY, y1s), (z_buf, NZ, z1s), (z_end, NY, z2s), (y_end, NZ, y2s), (ag_buf, NT, ags),
        (ys_buf, NY, ys1s), (zs_buf, NZ, zs1s), (ea_buf, NY * NH * NC, eas), (eb_buf, NX * NZ, ebs),
    ):
        wait(ref.at[pl.ds(0, count - 1)], sem)
    wait(zs_mid.at[pl.ds(0, NY // 2 - 1)], zs2s)
    wait(ys_mid.at[pl.ds(0, NZ // 2 - 1)], ys2s)

    @pl.when(team == 0)
    def _():
        wait(t_send, ts)

    @pl.when(team == 1)
    def _():
        wait(zs_mid.at[0], zs2s)
        wait(ys_mid.at[0], ys2s)
        wait(p_buf, ps)


def per_device(gradients, block_layer):
    return pl.pallas_call(
        body,
        out_shape=jax.ShapeDtypeStruct((1, ROWS, B), BF16),
        in_specs=[
            pl.BlockSpec(memory_space=pl.ANY),
            pl.BlockSpec(memory_space=pl.ANY),
        ],
        out_specs=pl.BlockSpec(memory_space=pltpu.VMEM),
        scratch_shapes=[
            pltpu.VMEM((B, B), BF16),
            pltpu.VMEM((B, B), F32),
            pltpu.VMEM((2, PACKED, T), F32),
            pltpu.VMEM((NZ, NY, VIA_Z, T), BF16),
            pltpu.VMEM((NY, NZ, VIA_Y, T), BF16),
            pltpu.VMEM((NZ, NY, VIA_Z, T), BF16),
            pltpu.VMEM((NY, NZ, VIA_Y, T), BF16),
            pltpu.VMEM((NY, VIA_Z, T), BF16),
            pltpu.VMEM((NZ, VIA_Y, T), BF16),
            pltpu.VMEM((NY, VIA_Z, T), BF16),
            pltpu.VMEM((NZ, VIA_Y, T), BF16),
            pltpu.VMEM((CHUNK, T), BF16),
            pltpu.VMEM((NT, CHUNK, T), BF16),
            pltpu.VMEM((NZ, NY // 2, COLS // 2, B), BF16),
            pltpu.VMEM((NY, NZ // 2, COLS // 2, B), BF16),
            pltpu.VMEM((NZ, NY // 2, COLS // 2, B), BF16),
            pltpu.VMEM((NY, NZ // 2, COLS // 2, B), BF16),
            pltpu.VMEM((NY // 2, COLS // 2, B), F32),
            pltpu.VMEM((NZ // 2, COLS // 2, B), F32),
            pltpu.VMEM((NY, COLS // 2, B), F32),
            pltpu.VMEM((NZ, COLS // 2, B), F32),
        ]
        + [pltpu.VMEM((B, B), F32)] * 5
        + [
            pltpu.VMEM((B, B), BF16),
            pltpu.VMEM((8 * NT, T), F32),
            pltpu.VMEM((8 * NT, T), F32),
            pltpu.VMEM((COLS, B), F32),
            pltpu.VMEM((ROWS, B), F32),
            pltpu.VMEM((1, T), F32),
            pltpu.VMEM((NY * NH * NC, 1, T), F32),
            pltpu.VMEM((1, T), F32),
            pltpu.VMEM((NX * NZ, 1, T), F32),
            pltpu.SMEM((1,), jnp.int32),
            pltpu.SemaphoreType.DMA((28,)),
        ],
        compiler_params=pltpu.CompilerParams(
            collective_id=0, has_side_effects=True, vmem_limit_bytes=60 * 1024 * 1024
        ),
    )(gradients, block_layer)


def solution(mesh):
    finer = Mesh(mesh.devices.reshape(NY, NZ, NX, NH, NC), AXES)
    return jax.shard_map(
        per_device,
        mesh=finer,
        in_specs=(P(("y", "z"), ("x", "h", "c"), None, None), P(("x", "h", "c"))),
        out_specs=P(("x", "h", "c"), ("y", "z"), None),
        check_vma=False,
    )
```

```python
import functools

import jax
import jax.numpy as jnp
from jax import lax
from jax.experimental import pallas as pl
from jax.experimental.pallas import tpu as pltpu
from jax.sharding import Mesh
from jax.sharding import PartitionSpec as P

LAYERS = 4
MESH_ID = pl.DeviceIdType.MESH
AXES = ("y", "z", "x", "h", "c")
NY, NZ, NX, NH, NC = 4, 8, 4, 2, 2
NP = NY * NZ
NT = NP // 2
B = 512
T = 128
NB = B // T
HALF = T // 2
PACKED = NB * (NB - 1) // 2 * T + NB * HALF + NB // 2 * HALF
CHUNK = PACKED // NT
VIA_Z = 32
VIA_Y = CHUNK - VIA_Z
COLS = B // NT
ROWS = B // NP
F32, BF16 = jnp.float32, jnp.bfloat16
DOT = functools.partial(lax.dot_general, preferred_element_type=F32)
NN = (((1,), (0,)), ((), ()))
NTR = (((1,), (1,)), ((), ()))


def split(x):
    high = x.astype(BF16)
    return high, (x - high.astype(F32)).astype(BF16)


def product(a, b):
    return DOT(a.astype(BF16), b.astype(BF16), NN)


def spread(size):
    return sorted(range(size), key=lambda d: -min(d, size - d))


def pairs_of(first, second):
    far = [(a, b) for a in spread(first) for b in spread(second)]
    return sorted(far, key=lambda p: -min(p[0], first - p[0]) - min(p[1], second - p[1]))


def body(
    g_hbm, layer_hbm, out_ref,
    g_ref, gt, packed, z_pack, y_pack, z_buf, y_buf, z_mid, y_mid, z_end, y_end,
    ag_send, ag_buf, zs_pack, ys_pack, zs_buf, ys_buf, zs_mid, ys_mid, zs_end, ys_end,
    stat, n0, n1, work, corr, root,
    t_send, t_buf, p_all, p_buf, ea_send, ea_buf, eb_send, eb_buf, layer_ref, sems,
):
    y, z, x = lax.axis_index("y"), lax.axis_index("z"), lax.axis_index("x")
    h, c = lax.axis_index("h"), lax.axis_index("c")
    team = (y + z) % 2
    member = y * (NZ // 2) + lax.div(z, 2)
    ys = [lax.rem(y + d, NY) for d in range(NY)]
    zs = [lax.rem(z + d, NZ) for d in range(NZ)]
    xs = [lax.rem(x + d, NX) for d in range(NX)]
    halves = [lax.rem(lax.div(z, 2) + d, NZ // 2) for d in range(NZ // 2)]
    (g_sem, z1s, z1r, y1s, y1r, z2s, z2r, y2s, y2r, ags, agr, zs1s, zs1r, ys1s, ys1r,
     zs2s, zs2r, ys2s, ys2r, ts, tr, ps, pr, eas, ear, ebs, ebr) = [sems.at[k] for k in range(27)]
    layer_sem = sems.at[27]

    def at(**place):
        where = {"y": y, "z": z, "x": x, "h": h, "c": c}
        where.update(place)
        return tuple(where[name] for name in AXES)

    def send(src, dst, send_sem, recv_sem, where):
        pltpu.make_async_remote_copy(
            src_ref=src, dst_ref=dst, send_sem=send_sem, recv_sem=recv_sem,
            device_id=where, device_id_type=MESH_ID,
        ).start()

    def wait(ref, sem):
        pltpu.make_async_copy(ref, ref, sem).wait()

    load = pltpu.make_async_copy(g_hbm.at[0, 0], g_ref, g_sem)
    load.start()
    load_layer = pltpu.make_async_copy(layer_hbm, layer_ref, layer_sem)
    load_layer.start()

    barrier = pltpu.get_barrier_semaphore()

    def greet(where):
        pl.semaphore_signal(barrier, inc=1, device_id=where, device_id_type=MESH_ID)

    for dy, dz in pairs_of(NY, NZ)[:-1]:
        greet(at(y=ys[dy], z=zs[dz]))
    for dx, dz in pairs_of(NX, NZ):
        if dx:
            greet(at(x=xs[dx], z=zs[dz]))
    for dy in spread(NY):
        greet(at(y=ys[dy], h=1 - h, c=c))
        greet(at(y=ys[dy], h=h, c=1 - c))
        greet(at(y=ys[dy], h=1 - h, c=1 - c))

    load.wait()
    load_layer.wait()
    g = g_ref[...]
    gt_value = g.T
    gt[...] = gt_value.astype(F32)
    for side, m in ((0, g), (1, gt_value)):
        row = 0
        corners = []
        for half in range(2):
            lo = half * (B // 2)
            panel = DOT(m[lo : lo + B // 2], m[lo:], NTR)
            for i in range(half * NB // 2, (half + 1) * NB // 2):
                for j in range(i, NB):
                    r, q = i * T - lo, j * T - lo
                    size = HALF if i == j else T
                    packed[side, row : row + size, :] = panel[r : r + size, q : q + T]
                    row += size
                    if i == j:
                        corners.append(panel[r + HALF : r + T, q : q + T])
        lane = lax.broadcasted_iota(jnp.int32, (HALF, T), 1)
        for k in range(0, NB, 2):
            packed[side, row : row + HALF, :] = jnp.where(
                lane < HALF, pltpu.roll(corners[k], HALF, 1), corners[k + 1]
            )
            row += HALF
    for yy in range(NY):
        for zz in range(NZ):
            side, first = (yy + zz) % 2, (yy * (NZ // 2) + zz // 2) * CHUNK
            z_pack[zz, yy] = packed[side, first : first + VIA_Z, :].astype(BF16)
            y_pack[yy, zz] = packed[side, first + VIA_Z : first + CHUNK, :].astype(BF16)

    pl.semaphore_wait(barrier, NP - 1 + 3 * NY + (NX - 1) * NZ)

    def along_y(source, target, send_sem, recv_sem):
        for d in spread(NY)[:-1]:
            send(source.at[ys[d]], target.at[y], send_sem, recv_sem, at(y=ys[d]))

    def along_z(source, target, send_sem, recv_sem):
        for d in spread(NZ)[:-1]:
            send(source.at[zs[d]], target.at[z], send_sem, recv_sem, at(z=zs[d]))

    def total(ref, count):
        result = ref[0].astype(F32)
        for k in range(1, count):
            result = result + ref[k].astype(F32)
        return result

    along_y(y_pack, y_buf, y1s, y1r)
    along_z(z_pack, z_buf, z1s, z1r)
    y_buf[y] = y_pack[y]
    z_buf[z] = z_pack[z]

    def columns(m, first):
        parts = [gt[T * q + 8 * m : T * q + 8 * m + 8, :] for q in range(first, first + NB // 2)]
        return jnp.concatenate(parts, axis=0).astype(BF16)

    for zz in range(NZ):
        for k in range(NY // 2):
            zs_pack[zz, k] = columns((zz % 2 + 2 * k) * (NZ // 2) + zz // 2, 0)
    for yy in range(NY):
        for k in range(NZ // 2):
            ys_pack[yy, k] = columns(yy * (NZ // 2) + k, NB // 2)
    ys_buf[y] = ys_pack[y]
    zs_buf[z] = zs_pack[z]

    along_y(ys_pack, ys_buf, ys1s, ys1r)
    along_z(zs_pack, zs_buf, zs1s, zs1r)

    wait(y_buf.at[pl.ds(0, NY - 1)], y1r)
    y_mid[...] = total(y_buf, NY).astype(BF16)
    along_z(y_mid, y_end, y2s, y2r)
    y_end[z] = y_mid[z]
    wait(z_buf.at[pl.ds(0, NZ - 1)], z1r)
    z_mid[...] = total(z_buf, NZ).astype(BF16)
    along_y(z_mid, z_end, z2s, z2r)
    z_end[y] = z_mid[y]
    wait(z_end.at[pl.ds(0, NY - 1)], z2r)
    wait(y_end.at[pl.ds(0, NZ - 1)], y2r)
    mine = jnp.concatenate([total(z_end, NY), total(y_end, NZ)], axis=0).astype(BF16)
    ag_send[...] = mine
    ag_buf[member] = mine

    for dy, dh in pairs_of(NY, NZ // 2)[:-1]:
        zz = 2 * halves[dh] + lax.rem(team + ys[dy], 2)
        send(ag_send, ag_buf.at[member], ags, agr, at(y=ys[dy], z=zz))

    wait(zs_buf.at[pl.ds(0, NZ - 1)], zs1r)
    zs_mid[...] = total(zs_buf, NZ)
    for k in range(NY // 2):
        yy = z % 2 + 2 * k

        @pl.when(yy != y)
        def _(k=k, yy=yy):
            send(zs_mid.at[k], zs_end.at[y], zs2s, zs2r, at(y=yy))

    wait(ys_buf.at[pl.ds(0, NY - 1)], ys1r)
    ys_mid[...] = total(ys_buf, NY)
    for k in range(NZ // 2):
        zz = y % 2 + 2 * k

        @pl.when(zz != z)
        def _(k=k, zz=zz):
            send(ys_mid.at[k], ys_end.at[z], ys2s, ys2r, at(z=zz))

    wait(ag_buf.at[pl.ds(0, NT - 1)], agr)

    whole = jnp.concatenate([ag_buf[k].astype(F32) for k in range(NT)], axis=0)
    row = 0
    spare = PACKED - NB // 2 * HALF
    lower = lax.broadcasted_iota(jnp.int32, (T, T), 0) >= HALF
    left = lax.broadcasted_iota(jnp.int32, (T, T), 1) < HALF
    for i in range(NB):
        for j in range(i, NB):
            if i == j:
                corner = whole[spare + i // 2 * HALF : spare + (i // 2 + 1) * HALF]
                corner = corner if i % 2 else pltpu.roll(corner, HALF, 1)
                block = jnp.concatenate([whole[row : row + HALF], corner], axis=0)
                block = jnp.where(lower & left, block.T, block)
                row += HALF
            else:
                block = whole[row : row + T]
                stat[j * T : (j + 1) * T, i * T : (i + 1) * T] = block.T
                row += T
            stat[i * T : (i + 1) * T, j * T : (j + 1) * T] = block
    eye = lax.broadcasted_iota(jnp.int32, (B, B), 0) == lax.broadcasted_iota(jnp.int32, (B, B), 1)
    s = stat[...]
    trace = jnp.sum(jnp.where(eye, s, 0.0), axis=(0, 1), keepdims=True)
    ridge = 0.01 * trace / B + 1e-06
    a = s + jnp.where(eye, ridge, 0.0)
    square = jnp.sum(a * a, axis=(0, 1), keepdims=True)
    scale = lax.rsqrt(square)
    n0[...] = a * (0.2 * scale)
    work[...] = product(n0[...], n0[...]) - 2.0 * n0[...]
    work[...] = product(work[...], work[...]) + 2.0 * work[...]
    n1[...] = 1.25**4 * (product(work[...], n0[...]) + n0[...])
    corr[...] = product(n0[...], n1[...]) - n0[...] - n1[...]
    work[...] = product(n1[...], n1[...]) - 2.0 * n1[...]
    work[...] = product(work[...], work[...]) + 2.0 * work[...]
    n0[...] = 1.25**4 * (product(work[...], n1[...]) + n1[...])
    factor = 1.25**3 * lax.rsqrt(jnp.sqrt(jnp.sqrt(square)))
    inverse = corr[...] - n0[...] - product(corr[...], n0[...])
    root[...] = (factor * (inverse + jnp.where(eye, 1.0, 0.0))).astype(BF16)

    @pl.when(team == 0)
    def _():
        wait(zs_end.at[pl.ds(0, NY - 1)], zs2r)
        wait(ys_end.at[pl.ds(0, NZ - 1)], ys2r)
        zs_end[y] = zs_mid[y // 2]
        ys_end[z] = ys_mid[z // 2]
        summed = jnp.concatenate([total(zs_end, NY), total(ys_end, NZ)], axis=0)
        high, low = split(summed)
        turned = DOT(high, root[...], NN) + DOT(low, root[...], NN)
        lane = lax.broadcasted_iota(jnp.int32, (8, T), 1) // COLS
        for e in range(NT):
            tile = jnp.zeros((8, T), F32)
            for q in range(NB):
                part = turned[8 * q : 8 * q + 8, T * (e // NB) : T * (e // NB) + T]
                shift = (COLS * (q - e % NB)) % T
                tile = jnp.where(lane == q, pltpu.roll(part, shift, 1) if shift else part, tile)
            t_send[8 * e : 8 * e + 8, :] = tile

        for dy, dh in pairs_of(NY, NZ // 2):
            e = ys[dy] * (NZ // 2) + halves[dh]
            send(
                t_send.at[pl.ds(pl.multiple_of(8 * e, 8), 8), :],
                t_buf.at[pl.ds(pl.multiple_of(8 * member, 8), 8), :],
                ts, tr, at(y=ys[dy], z=2 * halves[dh] + lax.rem(1 + ys[dy], 2)),
            )

        ea_send[...] = jnp.zeros((1, T), F32)

    @pl.when(team == 1)
    def _():
        wait(t_buf, tr)

    @pl.when(team == 1)
    def _():
        turned = t_buf[...].T
        rows = jnp.concatenate([turned[COLS * q : COLS * (q + 1), :] for q in range(NB)], axis=1)
        high, low = split(rows)
        p_all[...] = (DOT(high, root[...], NN) + DOT(low, root[...], NN)) / NP
        lane = lax.broadcasted_iota(jnp.int32, (1, T), 1)
        energy = jnp.sum(p_all[...] * p_all[...], axis=(0, 1), keepdims=True)
        here = layer_ref[0]
        ea_send[...] = jnp.where(lane == here, energy, 0.0) + jnp.where(
            lane == here + LAYERS, float(COLS * B), 0.0
        )

    place = (y * NH + h) * NC + c
    ea_buf[place] = ea_send[...]

    for hh in (1 - h, h):
        for dy in spread(NY):
            for cc in (1 - c, c):
                if not (hh is h and cc is c and dy == 0):
                    send(ea_send, ea_buf.at[place], eas, ear, at(y=ys[dy], h=hh, c=cc))

    @pl.when(team == 1)
    def _():
        partner = z + 1 - 2 * (z % 2)
        send(
            p_all.at[pl.ds(pl.multiple_of(ROWS * (partner % 2), ROWS), ROWS), :],
            p_buf, ps, pr, at(z=partner),
        )
        p_buf[...] = p_all[pl.ds(pl.multiple_of(ROWS * (z % 2), ROWS), ROWS), :]

    wait(ea_buf.at[pl.ds(0, NY * NH * NC - 1)], ear)
    eb_send[...] = jnp.sum(ea_buf[...], axis=0)
    spot = x * NZ + z
    eb_buf[spot] = eb_send[...]

    for dx, dz in pairs_of(NX, NZ)[:-1]:
        send(eb_send, eb_buf.at[spot], ebs, ebr, at(x=xs[dx], z=zs[dz]))

    @pl.when(team == 0)
    def _():
        wait(p_buf, pr)

    wait(eb_buf.at[pl.ds(0, NX * NZ - 1)], ebr)
    sums = jnp.sum(eb_buf[...], axis=0)
    lane = lax.broadcasted_iota(jnp.int32, (1, T), 1)
    here = layer_ref[0]
    layer_square = jnp.sum(jnp.where(lane == here, sums, 0.0), axis=1, keepdims=True)
    layer_count = jnp.sum(jnp.where(lane == here + LAYERS, sums, 0.0), axis=1, keepdims=True)
    out_ref[0] = (p_buf[...] * lax.rsqrt(layer_square / layer_count + 1e-06)).astype(BF16)

    for ref, count, sem in (
        (y_buf, NY, y1s), (z_buf, NZ, z1s), (z_end, NY, z2s), (y_end, NZ, y2s), (ag_buf, NT, ags),
        (ys_buf, NY, ys1s), (zs_buf, NZ, zs1s), (ea_buf, NY * NH * NC, eas), (eb_buf, NX * NZ, ebs),
    ):
        wait(ref.at[pl.ds(0, count - 1)], sem)
    wait(zs_mid.at[pl.ds(0, NY // 2 - 1)], zs2s)
    wait(ys_mid.at[pl.ds(0, NZ // 2 - 1)], ys2s)

    @pl.when(team == 0)
    def _():
        wait(t_send, ts)

    @pl.when(team == 1)
    def _():
        wait(zs_mid.at[0], zs2s)
        wait(ys_mid.at[0], ys2s)
        wait(p_buf, ps)


def per_device(gradients, block_layer):
    return pl.pallas_call(
        body,
        out_shape=pltpu.VMEM((1, ROWS, B), BF16),
        in_specs=[
            pl.BlockSpec(memory_space=pltpu.HBM),
            pl.BlockSpec(memory_space=pltpu.HBM),
        ],
        out_specs=pl.BlockSpec(memory_space=pltpu.VMEM),
        scratch_shapes=[
            pltpu.VMEM((B, B), BF16),
            pltpu.VMEM((B, B), F32),
            pltpu.VMEM((2, PACKED, T), F32),
            pltpu.VMEM((NZ, NY, VIA_Z, T), BF16),
            pltpu.VMEM((NY, NZ, VIA_Y, T), BF16),
            pltpu.VMEM((NZ, NY, VIA_Z, T), BF16),
            pltpu.VMEM((NY, NZ, VIA_Y, T), BF16),
            pltpu.VMEM((NY, VIA_Z, T), BF16),
            pltpu.VMEM((NZ, VIA_Y, T), BF16),
            pltpu.VMEM((NY, VIA_Z, T), BF16),
            pltpu.VMEM((NZ, VIA_Y, T), BF16),
            pltpu.VMEM((CHUNK, T), BF16),
            pltpu.VMEM((NT, CHUNK, T), BF16),
            pltpu.VMEM((NZ, NY // 2, COLS // 2, B), BF16),
            pltpu.VMEM((NY, NZ // 2, COLS // 2, B), BF16),
            pltpu.VMEM((NZ, NY // 2, COLS // 2, B), BF16),
            pltpu.VMEM((NY, NZ // 2, COLS // 2, B), BF16),
            pltpu.VMEM((NY // 2, COLS // 2, B), F32),
            pltpu.VMEM((NZ // 2, COLS // 2, B), F32),
            pltpu.VMEM((NY, COLS // 2, B), F32),
            pltpu.VMEM((NZ, COLS // 2, B), F32),
        ]
        + [pltpu.VMEM((B, B), F32)] * 5
        + [
            pltpu.VMEM((B, B), BF16),
            pltpu.VMEM((8 * NT, T), F32),
            pltpu.VMEM((8 * NT, T), F32),
            pltpu.VMEM((COLS, B), F32),
            pltpu.VMEM((ROWS, B), F32),
            pltpu.VMEM((1, T), F32),
            pltpu.VMEM((NY * NH * NC, 1, T), F32),
            pltpu.VMEM((1, T), F32),
            pltpu.VMEM((NX * NZ, 1, T), F32),
            pltpu.SMEM((1,), jnp.int32),
            pltpu.SemaphoreType.DMA((28,)),
        ],
        compiler_params=pltpu.CompilerParams(
            collective_id=0, has_side_effects=True, vmem_limit_bytes=60 * 1024 * 1024
        ),
    )(gradients, block_layer)


def solution(mesh):
    finer = Mesh(mesh.devices.reshape(NY, NZ, NX, NH, NC), AXES)
    return jax.shard_map(
        per_device,
        mesh=finer,
        in_specs=(P(("y", "z"), ("x", "h", "c"), None, None), P(("x", "h", "c"))),
        out_specs=P(("x", "h", "c"), ("y", "z"), None),
        check_vma=False,
    )
```

```python
import functools

import jax
import jax.numpy as jnp
from jax import lax
from jax.experimental import pallas as pl
from jax.experimental.pallas import tpu as pltpu
from jax.sharding import Mesh
from jax.sharding import PartitionSpec as P

LAYERS = 4
MESH_ID = pl.DeviceIdType.MESH
AXES = ("y", "z", "x", "h", "c")
NY, NZ, NX, NH, NC = 4, 8, 4, 2, 2
NP = NY * NZ
NT = NP // 2
B = 512
T = 128
NB = B // T
HALF = T // 2
PACKED = NB * (NB - 1) // 2 * T + NB * HALF + NB // 2 * HALF
CHUNK = PACKED // NT
VIA_Z = 32
VIA_Y = CHUNK - VIA_Z
COLS = B // NT
ROWS = B // NP
F32, BF16 = jnp.float32, jnp.bfloat16
DOT = functools.partial(lax.dot_general, preferred_element_type=F32)
NN = (((1,), (0,)), ((), ()))
NTR = (((1,), (1,)), ((), ()))


def stacked(x):
    high = x.astype(BF16)
    return jnp.concatenate([high, (x - high.astype(F32)).astype(BF16)], axis=0)


def product(a, b):
    return DOT(a.astype(BF16), b.astype(BF16), NN)


def spread(size):
    return sorted(range(size), key=lambda d: -min(d, size - d))


def pairs_of(first, second):
    far = [(a, b) for a in spread(first) for b in spread(second)]
    return sorted(far, key=lambda p: -min(p[0], first - p[0]) - min(p[1], second - p[1]))


def body(
    g_hbm, layer_hbm, out_ref,
    g_ref, gt, packed, z_pack, y_pack, z_buf, y_buf, z_mid, y_mid, z_end, y_end,
    ag_send, ag_buf, zs_pack, ys_pack, zs_buf, ys_buf, zs_mid, ys_mid, zs_end, ys_end,
    n0, n1, work, corr, root,
    t_send, t_buf, p_all, p_buf, ea_send, ea_buf, eb_send, eb_buf, layer_ref, sems,
):
    y, z, x = lax.axis_index("y"), lax.axis_index("z"), lax.axis_index("x")
    h, c = lax.axis_index("h"), lax.axis_index("c")
    team = (y + z) % 2
    member = y * (NZ // 2) + lax.div(z, 2)
    ys = [lax.rem(y + d, NY) for d in range(NY)]
    zs = [lax.rem(z + d, NZ) for d in range(NZ)]
    xs = [lax.rem(x + d, NX) for d in range(NX)]
    halves = [lax.rem(lax.div(z, 2) + d, NZ // 2) for d in range(NZ // 2)]
    (g_sem, z1s, z1r, y1s, y1r, z2s, z2r, y2s, y2r, ags, agr, zs1s, zs1r, ys1s, ys1r,
     zs2s, zs2r, ys2s, ys2r, ts, tr, ps, pr, eas, ear, ebs, ebr) = [sems.at[k] for k in range(27)]
    layer_sem = sems.at[27]

    def at(**place):
        where = {"y": y, "z": z, "x": x, "h": h, "c": c}
        where.update(place)
        return tuple(where[name] for name in AXES)

    def send(src, dst, send_sem, recv_sem, where):
        pltpu.make_async_remote_copy(
            src_ref=src, dst_ref=dst, send_sem=send_sem, recv_sem=recv_sem,
            device_id=where, device_id_type=MESH_ID,
        ).start()

    def wait(ref, sem):
        pltpu.make_async_copy(ref, ref, sem).wait()

    load = pltpu.make_async_copy(g_hbm.at[0, 0], g_ref, g_sem)
    load.start()
    load_layer = pltpu.make_async_copy(layer_hbm, layer_ref, layer_sem)
    load_layer.start()

    barrier = pltpu.get_barrier_semaphore()

    def greet(where):
        pl.semaphore_signal(barrier, inc=1, device_id=where, device_id_type=MESH_ID)

    for dx, dz in pairs_of(NX, NZ):
        if dx:
            greet(at(x=xs[dx], z=zs[dz]))
    for dy in spread(NY):
        greet(at(y=ys[dy], h=1 - h, c=c))
        greet(at(y=ys[dy], h=h, c=1 - c))
        greet(at(y=ys[dy], h=1 - h, c=1 - c))
    for dy, dz in pairs_of(NY, NZ)[:-1]:
        greet(at(y=ys[dy], z=zs[dz]))

    load.wait()
    load_layer.wait()
    g = g_ref[...]
    gt_value = g.T
    gt[...] = gt_value.astype(F32)
    for side, m in ((0, g), (1, gt_value)):
        row = 0
        corners = []
        for half in range(2):
            lo = half * (B // 2)
            panel = DOT(m[lo : lo + B // 2], m[lo:], NTR)
            for i in range(half * NB // 2, (half + 1) * NB // 2):
                for j in range(i, NB):
                    r, q = i * T - lo, j * T - lo
                    size = HALF if i == j else T
                    packed[side, row : row + size, :] = panel[r : r + size, q : q + T]
                    row += size
                    if i == j:
                        corners.append(panel[r + HALF : r + T, q : q + T])
        lane = lax.broadcasted_iota(jnp.int32, (HALF, T), 1)
        for k in range(0, NB, 2):
            packed[side, row : row + HALF, :] = jnp.where(
                lane < HALF, pltpu.roll(corners[k], HALF, 1), corners[k + 1]
            )
            row += HALF
    for yy in range(NY):
        for zz in range(NZ):
            side, first = (yy + zz) % 2, (yy * (NZ // 2) + zz // 2) * CHUNK
            z_pack[zz, yy] = packed[side, first : first + VIA_Z, :].astype(BF16)
            y_pack[yy, zz] = packed[side, first + VIA_Z : first + CHUNK, :].astype(BF16)

    pl.semaphore_wait(barrier, NP - 1 + 3 * NY + (NX - 1) * NZ)

    def along_y(source, target, send_sem, recv_sem):
        for d in spread(NY)[:-1]:
            send(source.at[ys[d]], target.at[y], send_sem, recv_sem, at(y=ys[d]))

    def along_z(source, target, send_sem, recv_sem):
        for d in spread(NZ)[:-1]:
            send(source.at[zs[d]], target.at[z], send_sem, recv_sem, at(z=zs[d]))

    def total(ref, count):
        result = ref[0].astype(F32)
        for k in range(1, count):
            result = result + ref[k].astype(F32)
        return result

    along_y(y_pack, y_buf, y1s, y1r)
    along_z(z_pack, z_buf, z1s, z1r)
    y_buf[y] = y_pack[y]
    z_buf[z] = z_pack[z]

    def columns(m, first):
        parts = [gt[T * q + 8 * m : T * q + 8 * m + 8, :] for q in range(first, first + NB // 2)]
        return jnp.concatenate(parts, axis=0).astype(BF16)

    for zz in range(NZ):
        for k in range(NY // 2):
            zs_pack[zz, k] = columns((zz % 2 + 2 * k) * (NZ // 2) + zz // 2, 0)
    for yy in range(NY):
        for k in range(NZ // 2):
            ys_pack[yy, k] = columns(yy * (NZ // 2) + k, NB // 2)
    ys_buf[y] = ys_pack[y]
    zs_buf[z] = zs_pack[z]

    along_y(ys_pack, ys_buf, ys1s, ys1r)
    along_z(zs_pack, zs_buf, zs1s, zs1r)

    wait(y_buf.at[pl.ds(0, NY - 1)], y1r)
    y_mid[...] = total(y_buf, NY).astype(BF16)
    along_z(y_mid, y_end, y2s, y2r)
    y_end[z] = y_mid[z]
    wait(z_buf.at[pl.ds(0, NZ - 1)], z1r)
    z_mid[...] = total(z_buf, NZ).astype(BF16)
    along_y(z_mid, z_end, z2s, z2r)
    z_end[y] = z_mid[y]
    wait(z_end.at[pl.ds(0, NY - 1)], z2r)
    wait(y_end.at[pl.ds(0, NZ - 1)], y2r)
    mine = jnp.concatenate([total(z_end, NY), total(y_end, NZ)], axis=0).astype(BF16)
    ag_send[...] = mine
    ag_buf[member] = mine

    for dy, dh in pairs_of(NY, NZ // 2)[:-1]:
        zz = 2 * halves[dh] + lax.rem(team + ys[dy], 2)
        send(ag_send, ag_buf.at[member], ags, agr, at(y=ys[dy], z=zz))

    wait(zs_buf.at[pl.ds(0, NZ - 1)], zs1r)
    zs_mid[...] = total(zs_buf, NZ)
    for k in range(NY // 2):
        yy = z % 2 + 2 * k

        @pl.when(yy != y)
        def _(k=k, yy=yy):
            send(zs_mid.at[k], zs_end.at[y], zs2s, zs2r, at(y=yy))

    wait(ys_buf.at[pl.ds(0, NY - 1)], ys1r)
    ys_mid[...] = total(ys_buf, NY)
    for k in range(NZ // 2):
        zz = y % 2 + 2 * k

        @pl.when(zz != z)
        def _(k=k, zz=zz):
            send(ys_mid.at[k], ys_end.at[z], ys2s, ys2r, at(z=zz))

    wait(ag_buf.at[pl.ds(0, NT - 1)], agr)

    whole = jnp.concatenate([ag_buf[k].astype(F32) for k in range(NT)], axis=0)
    spare = PACKED - NB // 2 * HALF
    diagonal, off_diagonal, corners = [], {}, []
    row = 0
    for i in range(NB):
        for j in range(i, NB):
            if i == j:
                diagonal.append(whole[row : row + HALF])
                row += HALF
            else:
                off_diagonal[i, j] = whole[row : row + T]
                row += T
    for i in range(NB // 2):
        corners.append(whole[spare + i * HALF : spare + (i + 1) * HALF])
    down = lax.broadcasted_iota(jnp.int32, (HALF, T), 0)
    across = lax.broadcasted_iota(jnp.int32, (HALF, T), 1)

    def added(x):
        return jnp.sum(x.reshape(-1, 8, T), axis=0)

    squares = sum(2.0 * added(block * block) for block in off_diagonal.values())
    squares += sum(added(jnp.where(across < HALF, 1.0, 2.0) * block * block) for block in diagonal)
    squares += sum(added(block * block) for block in corners)
    traces = sum(added(jnp.where(across == down, block, 0.0)) for block in diagonal)
    traces += sum(added(jnp.where(across % HALF == down, block, 0.0)) for block in corners)
    trace = jnp.sum(traces, axis=(0, 1), keepdims=True)
    ridge = 0.01 * trace / B + 1e-06
    square = jnp.sum(squares, axis=(0, 1), keepdims=True) + ridge * (2.0 * trace + B * ridge)
    scale = 0.2 * lax.rsqrt(square)
    lower = lax.broadcasted_iota(jnp.int32, (T, T), 0) >= HALF
    left = lax.broadcasted_iota(jnp.int32, (T, T), 1) < HALF
    unit = lax.broadcasted_iota(jnp.int32, (T, T), 0) == lax.broadcasted_iota(jnp.int32, (T, T), 1)
    for (i, j), block in off_diagonal.items():
        block = block * scale
        n0[i * T : (i + 1) * T, j * T : (j + 1) * T] = block
        n0[j * T : (j + 1) * T, i * T : (i + 1) * T] = block.T
    for i in range(NB):
        corner = corners[i // 2] if i % 2 else pltpu.roll(corners[i // 2], HALF, 1)
        block = jnp.concatenate([diagonal[i], corner], axis=0)
        block = jnp.where(lower & left, block.T, block)
        n0[i * T : (i + 1) * T, i * T : (i + 1) * T] = (block + jnp.where(unit, ridge, 0.0)) * scale
    eye = lax.broadcasted_iota(jnp.int32, (B, B), 0) == lax.broadcasted_iota(jnp.int32, (B, B), 1)
    work[...] = product(n0[...], n0[...]) - 2.0 * n0[...]
    work[...] = product(work[...], work[...]) + 2.0 * work[...]
    n1[...] = 1.25**4 * (product(work[...], n0[...]) + n0[...])
    corr[...] = product(n0[...], n1[...]) - n0[...] - n1[...]
    work[...] = product(n1[...], n1[...]) - 2.0 * n1[...]
    work[...] = product(work[...], work[...]) + 2.0 * work[...]
    n0[...] = 1.25**4 * (product(work[...], n1[...]) + n1[...])
    factor = 1.25**3 * lax.rsqrt(jnp.sqrt(jnp.sqrt(square)))
    inverse = corr[...] - n0[...] - product(corr[...], n0[...])
    root[...] = (factor * (inverse + jnp.where(eye, 1.0, 0.0))).astype(BF16)

    @pl.when(team == 0)
    def _():
        wait(zs_end.at[pl.ds(0, NY - 1)], zs2r)
        wait(ys_end.at[pl.ds(0, NZ - 1)], ys2r)
        zs_end[y] = zs_mid[y // 2]
        ys_end[z] = ys_mid[z // 2]
        summed = jnp.concatenate([total(zs_end, NY), total(ys_end, NZ)], axis=0)
        both = DOT(stacked(summed), root[...], NN)
        turned = both[:COLS] + both[COLS:]
        lane = lax.broadcasted_iota(jnp.int32, (8, T), 1) // COLS
        for e in range(NT):
            tile = jnp.zeros((8, T), F32)
            for q in range(NB):
                part = turned[8 * q : 8 * q + 8, T * (e // NB) : T * (e // NB) + T]
                shift = (COLS * (q - e % NB)) % T
                tile = jnp.where(lane == q, pltpu.roll(part, shift, 1) if shift else part, tile)
            t_send[8 * e : 8 * e + 8, :] = tile

        for dy, dh in pairs_of(NY, NZ // 2):
            e = ys[dy] * (NZ // 2) + halves[dh]
            send(
                t_send.at[pl.ds(pl.multiple_of(8 * e, 8), 8), :],
                t_buf.at[pl.ds(pl.multiple_of(8 * member, 8), 8), :],
                ts, tr, at(y=ys[dy], z=2 * halves[dh] + lax.rem(1 + ys[dy], 2)),
            )

        ea_send[...] = jnp.zeros((1, T), F32)

    @pl.when(team == 1)
    def _():
        wait(t_buf, tr)

    @pl.when(team == 1)
    def _():
        turned = t_buf[...].T
        rows = jnp.concatenate([turned[COLS * q : COLS * (q + 1), :] for q in range(NB)], axis=1)
        both = DOT(stacked(rows), root[...], NN)
        p_all[...] = (both[:COLS] + both[COLS:]) * (1.0 / NP)
        lane = lax.broadcasted_iota(jnp.int32, (1, T), 1)
        energy = jnp.sum(p_all[...] * p_all[...], axis=(0, 1), keepdims=True)
        here = layer_ref[0]
        ea_send[...] = jnp.where(lane == here, energy, 0.0) + jnp.where(
            lane == here + LAYERS, float(COLS * B), 0.0
        )

    place = (y * NH + h) * NC + c
    ea_buf[place] = ea_send[...]

    for hh in (1 - h, h):
        for dy in spread(NY):
            for cc in (1 - c, c):
                if not (hh is h and cc is c and dy == 0):
                    send(ea_send, ea_buf.at[place], eas, ear, at(y=ys[dy], h=hh, c=cc))

    @pl.when(team == 1)
    def _():
        partner = z + 1 - 2 * (z % 2)
        send(
            p_all.at[pl.ds(pl.multiple_of(ROWS * (partner % 2), ROWS), ROWS), :],
            p_buf, ps, pr, at(z=partner),
        )
        p_buf[...] = p_all[pl.ds(pl.multiple_of(ROWS * (z % 2), ROWS), ROWS), :]

    wait(ea_buf.at[pl.ds(0, NY * NH * NC - 1)], ear)
    eb_send[...] = jnp.sum(ea_buf[...], axis=0)
    spot = x * NZ + z
    eb_buf[spot] = eb_send[...]

    for dx, dz in pairs_of(NX, NZ)[:-1]:
        send(eb_send, eb_buf.at[spot], ebs, ebr, at(x=xs[dx], z=zs[dz]))

    @pl.when(team == 0)
    def _():
        wait(p_buf, pr)

    wait(eb_buf.at[pl.ds(0, NX * NZ - 1)], ebr)
    sums = jnp.sum(eb_buf[...], axis=0)
    lane = lax.broadcasted_iota(jnp.int32, (1, T), 1)
    here = layer_ref[0]
    layer_square = jnp.sum(jnp.where(lane == here, sums, 0.0), axis=1, keepdims=True)
    layer_count = jnp.sum(jnp.where(lane == here + LAYERS, sums, 0.0), axis=1, keepdims=True)
    out_ref[0] = (p_buf[...] * lax.rsqrt(layer_square / layer_count + 1e-06)).astype(BF16)

    for ref, count, sem in (
        (y_buf, NY, y1s), (z_buf, NZ, z1s), (z_end, NY, z2s), (y_end, NZ, y2s), (ag_buf, NT, ags),
        (ys_buf, NY, ys1s), (zs_buf, NZ, zs1s), (ea_buf, NY * NH * NC, eas), (eb_buf, NX * NZ, ebs),
    ):
        wait(ref.at[pl.ds(0, count - 1)], sem)
    wait(zs_mid.at[pl.ds(0, NY // 2 - 1)], zs2s)
    wait(ys_mid.at[pl.ds(0, NZ // 2 - 1)], ys2s)

    @pl.when(team == 0)
    def _():
        wait(t_send, ts)

    @pl.when(team == 1)
    def _():
        wait(zs_mid.at[0], zs2s)
        wait(ys_mid.at[0], ys2s)
        wait(p_buf, ps)


def per_device(gradients, block_layer):
    return pl.pallas_call(
        body,
        out_shape=pltpu.VMEM((1, ROWS, B), BF16),
        in_specs=[
            pl.BlockSpec(memory_space=pltpu.HBM),
            pl.BlockSpec(memory_space=pltpu.HBM),
        ],
        out_specs=pl.BlockSpec(memory_space=pltpu.VMEM),
        scratch_shapes=[
            pltpu.VMEM((B, B), BF16),
            pltpu.VMEM((B, B), F32),
            pltpu.VMEM((2, PACKED, T), F32),
            pltpu.VMEM((NZ, NY, VIA_Z, T), BF16),
            pltpu.VMEM((NY, NZ, VIA_Y, T), BF16),
            pltpu.VMEM((NZ, NY, VIA_Z, T), BF16),
            pltpu.VMEM((NY, NZ, VIA_Y, T), BF16),
            pltpu.VMEM((NY, VIA_Z, T), BF16),
            pltpu.VMEM((NZ, VIA_Y, T), BF16),
            pltpu.VMEM((NY, VIA_Z, T), BF16),
            pltpu.VMEM((NZ, VIA_Y, T), BF16),
            pltpu.VMEM((CHUNK, T), BF16),
            pltpu.VMEM((NT, CHUNK, T), BF16),
            pltpu.VMEM((NZ, NY // 2, COLS // 2, B), BF16),
            pltpu.VMEM((NY, NZ // 2, COLS // 2, B), BF16),
            pltpu.VMEM((NZ, NY // 2, COLS // 2, B), BF16),
            pltpu.VMEM((NY, NZ // 2, COLS // 2, B), BF16),
            pltpu.VMEM((NY // 2, COLS // 2, B), F32),
            pltpu.VMEM((NZ // 2, COLS // 2, B), F32),
            pltpu.VMEM((NY, COLS // 2, B), F32),
            pltpu.VMEM((NZ, COLS // 2, B), F32),
        ]
        + [pltpu.VMEM((B, B), F32)] * 4
        + [
            pltpu.VMEM((B, B), BF16),
            pltpu.VMEM((8 * NT, T), F32),
            pltpu.VMEM((8 * NT, T), F32),
            pltpu.VMEM((COLS, B), F32),
            pltpu.VMEM((ROWS, B), F32),
            pltpu.VMEM((1, T), F32),
            pltpu.VMEM((NY * NH * NC, 1, T), F32),
            pltpu.VMEM((1, T), F32),
            pltpu.VMEM((NX * NZ, 1, T), F32),
            pltpu.SMEM((1,), jnp.int32),
            pltpu.SemaphoreType.DMA((28,)),
        ],
        compiler_params=pltpu.CompilerParams(
            collective_id=0, has_side_effects=True, vmem_limit_bytes=60 * 1024 * 1024
        ),
    )(gradients, block_layer)


def solution(mesh):
    finer = Mesh(mesh.devices.reshape(NY, NZ, NX, NH, NC), AXES)
    return jax.shard_map(
        per_device,
        mesh=finer,
        in_specs=(P(("y", "z"), ("x", "h", "c"), None, None), P(("x", "h", "c"))),
        out_specs=P(("x", "h", "c"), ("y", "z"), None),
        check_vma=False,
    )
```

```python
import functools

import jax
import jax.numpy as jnp
from jax import lax
from jax.experimental import pallas as pl
from jax.experimental.pallas import tpu as pltpu
from jax.sharding import Mesh
from jax.sharding import PartitionSpec as P

LAYERS = 4
MESH_ID = pl.DeviceIdType.MESH
AXES = ("y", "z", "x", "h", "c")
NY, NZ, NX, NH, NC = 4, 8, 4, 2, 2
NP = NY * NZ
NT = NP // 2
B = 512
T = 128
NB = B // T
HALF = T // 2
PACKED = NB * (NB - 1) // 2 * T + NB * HALF + NB // 2 * HALF
CHUNK = PACKED // NT
VIA_Z = 32
VIA_Y = CHUNK - VIA_Z
COLS = B // NT
ROWS = B // NP
F32, BF16 = jnp.float32, jnp.bfloat16
DOT = functools.partial(lax.dot_general, preferred_element_type=F32)
NN = (((1,), (0,)), ((), ()))
NTR = (((1,), (1,)), ((), ()))


def stacked(x):
    high = x.astype(BF16)
    return jnp.concatenate([high, (x - high.astype(F32)).astype(BF16)], axis=0)


def spread(size):
    return sorted(range(size), key=lambda d: -min(d, size - d))


def pairs_of(first, second):
    far = [(a, b) for a in spread(first) for b in spread(second)]
    return sorted(far, key=lambda p: -min(p[0], first - p[0]) - min(p[1], second - p[1]))


def body(
    g_hbm, layer_hbm, out_ref,
    g_ref, gt, packed, z_pack, y_pack, z_buf, y_buf, z_mid, y_mid, z_end, y_end,
    ag_send, ag_buf, zs_pack, ys_pack, zs_buf, ys_buf, zs_mid, ys_mid, zs_end, ys_end,
    n0, n1, work, corr, thin, term, root,
    t_send, t_buf, p_all, p_buf, ea_send, ea_buf, eb_send, eb_buf, layer_ref, sems,
):
    y, z, x = lax.axis_index("y"), lax.axis_index("z"), lax.axis_index("x")
    h, c = lax.axis_index("h"), lax.axis_index("c")
    team = (y + z) % 2
    member = y * (NZ // 2) + lax.div(z, 2)
    ys = [lax.rem(y + d, NY) for d in range(NY)]
    zs = [lax.rem(z + d, NZ) for d in range(NZ)]
    xs = [lax.rem(x + d, NX) for d in range(NX)]
    halves = [lax.rem(lax.div(z, 2) + d, NZ // 2) for d in range(NZ // 2)]
    (g_sem, z1s, z1r, y1s, y1r, z2s, z2r, y2s, y2r, ags, agr, zs1s, zs1r, ys1s, ys1r,
     zs2s, zs2r, ys2s, ys2r, ts, tr, ps, pr, eas, ear, ebs, ebr) = [sems.at[k] for k in range(27)]
    layer_sem = sems.at[27]

    def at(**place):
        where = {"y": y, "z": z, "x": x, "h": h, "c": c}
        where.update(place)
        return tuple(where[name] for name in AXES)

    def send(src, dst, send_sem, recv_sem, where):
        pltpu.make_async_remote_copy(
            src_ref=src, dst_ref=dst, send_sem=send_sem, recv_sem=recv_sem,
            device_id=where, device_id_type=MESH_ID,
        ).start()

    def wait(ref, sem):
        pltpu.make_async_copy(ref, ref, sem).wait()

    load = pltpu.make_async_copy(g_hbm.at[0, 0], g_ref, g_sem)
    load.start()
    load_layer = pltpu.make_async_copy(layer_hbm, layer_ref, layer_sem)
    load_layer.start()

    barrier = pltpu.get_barrier_semaphore()

    def greet(where):
        pl.semaphore_signal(barrier, inc=1, device_id=where, device_id_type=MESH_ID)

    for dx, dz in pairs_of(NX, NZ):
        if dx:
            greet(at(x=xs[dx], z=zs[dz]))
    for dy in spread(NY):
        greet(at(y=ys[dy], h=1 - h, c=c))
        greet(at(y=ys[dy], h=h, c=1 - c))
        greet(at(y=ys[dy], h=1 - h, c=1 - c))
    for dy, dz in pairs_of(NY, NZ)[:-1]:
        greet(at(y=ys[dy], z=zs[dz]))

    load.wait()
    load_layer.wait()
    g = g_ref[...]
    gt_value = g.T
    gt[...] = gt_value.astype(F32)
    for side, m in ((0, g), (1, gt_value)):
        row = 0
        corners = []
        for half in range(2):
            lo = half * (B // 2)
            panel = DOT(m[lo : lo + B // 2], m[lo:], NTR)
            for i in range(half * NB // 2, (half + 1) * NB // 2):
                for j in range(i, NB):
                    r, q = i * T - lo, j * T - lo
                    size = HALF if i == j else T
                    packed[side, row : row + size, :] = panel[r : r + size, q : q + T]
                    row += size
                    if i == j:
                        corners.append(panel[r + HALF : r + T, q : q + T])
        lane = lax.broadcasted_iota(jnp.int32, (HALF, T), 1)
        for k in range(0, NB, 2):
            packed[side, row : row + HALF, :] = jnp.where(
                lane < HALF, pltpu.roll(corners[k], HALF, 1), corners[k + 1]
            )
            row += HALF
    for yy in range(NY):
        for zz in range(NZ):
            side, first = (yy + zz) % 2, (yy * (NZ // 2) + zz // 2) * CHUNK
            z_pack[zz, yy] = packed[side, first : first + VIA_Z, :].astype(BF16)
            y_pack[yy, zz] = packed[side, first + VIA_Z : first + CHUNK, :].astype(BF16)

    pl.semaphore_wait(barrier, NP - 1 + 3 * NY + (NX - 1) * NZ)

    def along_y(source, target, send_sem, recv_sem):
        for d in spread(NY)[:-1]:
            send(source.at[ys[d]], target.at[y], send_sem, recv_sem, at(y=ys[d]))

    def along_z(source, target, send_sem, recv_sem):
        for d in spread(NZ)[:-1]:
            send(source.at[zs[d]], target.at[z], send_sem, recv_sem, at(z=zs[d]))

    def total(ref, count):
        result = ref[0].astype(F32)
        for k in range(1, count):
            result = result + ref[k].astype(F32)
        return result

    along_y(y_pack, y_buf, y1s, y1r)
    along_z(z_pack, z_buf, z1s, z1r)
    y_buf[y] = y_pack[y]
    z_buf[z] = z_pack[z]

    def columns(m, first):
        parts = [gt[T * q + 8 * m : T * q + 8 * m + 8, :] for q in range(first, first + NB // 2)]
        return jnp.concatenate(parts, axis=0).astype(BF16)

    for zz in range(NZ):
        for k in range(NY // 2):
            zs_pack[zz, k] = columns((zz % 2 + 2 * k) * (NZ // 2) + zz // 2, 0)
    for yy in range(NY):
        for k in range(NZ // 2):
            ys_pack[yy, k] = columns(yy * (NZ // 2) + k, NB // 2)
    ys_buf[y] = ys_pack[y]
    zs_buf[z] = zs_pack[z]

    along_y(ys_pack, ys_buf, ys1s, ys1r)
    along_z(zs_pack, zs_buf, zs1s, zs1r)

    wait(y_buf.at[pl.ds(0, NY - 1)], y1r)
    y_mid[...] = total(y_buf, NY).astype(BF16)
    along_z(y_mid, y_end, y2s, y2r)
    y_end[z] = y_mid[z]
    wait(z_buf.at[pl.ds(0, NZ - 1)], z1r)
    z_mid[...] = total(z_buf, NZ).astype(BF16)
    along_y(z_mid, z_end, z2s, z2r)
    z_end[y] = z_mid[y]
    wait(z_end.at[pl.ds(0, NY - 1)], z2r)
    wait(y_end.at[pl.ds(0, NZ - 1)], y2r)
    mine = jnp.concatenate([total(z_end, NY), total(y_end, NZ)], axis=0).astype(BF16)
    ag_send[...] = mine
    ag_buf[member] = mine

    for dy, dh in pairs_of(NY, NZ // 2)[:-1]:
        zz = 2 * halves[dh] + lax.rem(team + ys[dy], 2)
        send(ag_send, ag_buf.at[member], ags, agr, at(y=ys[dy], z=zz))

    wait(zs_buf.at[pl.ds(0, NZ - 1)], zs1r)
    zs_mid[...] = total(zs_buf, NZ)
    for k in range(NY // 2):
        yy = z % 2 + 2 * k

        @pl.when(yy != y)
        def _(k=k, yy=yy):
            send(zs_mid.at[k], zs_end.at[y], zs2s, zs2r, at(y=yy))

    wait(ys_buf.at[pl.ds(0, NY - 1)], ys1r)
    ys_mid[...] = total(ys_buf, NY)
    for k in range(NZ // 2):
        zz = y % 2 + 2 * k

        @pl.when(zz != z)
        def _(k=k, zz=zz):
            send(ys_mid.at[k], ys_end.at[z], ys2s, ys2r, at(z=zz))

    wait(ag_buf.at[pl.ds(0, NT - 1)], agr)

    whole = jnp.concatenate([ag_buf[k].astype(F32) for k in range(NT)], axis=0)
    spare = PACKED - NB // 2 * HALF
    diagonal, off_diagonal, corners = [], {}, []
    row = 0
    for i in range(NB):
        for j in range(i, NB):
            if i == j:
                diagonal.append(whole[row : row + HALF])
                row += HALF
            else:
                off_diagonal[i, j] = whole[row : row + T]
                row += T
    for i in range(NB // 2):
        corners.append(whole[spare + i * HALF : spare + (i + 1) * HALF])
    down = lax.broadcasted_iota(jnp.int32, (HALF, T), 0)
    across = lax.broadcasted_iota(jnp.int32, (HALF, T), 1)

    def added(x):
        return jnp.sum(x.reshape(-1, 8, T), axis=0)

    squares = sum(2.0 * added(block * block) for block in off_diagonal.values())
    squares += sum(added(jnp.where(across < HALF, 1.0, 2.0) * block * block) for block in diagonal)
    squares += sum(added(block * block) for block in corners)
    traces = sum(added(jnp.where(across == down, block, 0.0)) for block in diagonal)
    traces += sum(added(jnp.where(across % HALF == down, block, 0.0)) for block in corners)
    trace = jnp.sum(traces, axis=(0, 1), keepdims=True)
    ridge = 0.01 * trace / B + 1e-06
    square = jnp.sum(squares, axis=(0, 1), keepdims=True) + ridge * (2.0 * trace + B * ridge)
    scale = 0.2 * lax.rsqrt(square)
    lower = lax.broadcasted_iota(jnp.int32, (T, T), 0) >= HALF
    left = lax.broadcasted_iota(jnp.int32, (T, T), 1) < HALF
    unit = lax.broadcasted_iota(jnp.int32, (T, T), 0) == lax.broadcasted_iota(jnp.int32, (T, T), 1)
    for (i, j), block in off_diagonal.items():
        block = block * scale
        n0[i * T : (i + 1) * T, j * T : (j + 1) * T] = block
        n0[j * T : (j + 1) * T, i * T : (i + 1) * T] = block.T
    for i in range(NB):
        corner = corners[i // 2] if i % 2 else pltpu.roll(corners[i // 2], HALF, 1)
        block = jnp.concatenate([diagonal[i], corner], axis=0)
        block = jnp.where(lower & left, block.T, block)
        n0[i * T : (i + 1) * T, i * T : (i + 1) * T] = (block + jnp.where(unit, ridge, 0.0)) * scale
    eye = lax.broadcasted_iota(jnp.int32, (B, B), 0) == lax.broadcasted_iota(jnp.int32, (B, B), 1)
    thin0, thin1 = thin.at[:B], thin.at[B:]
    thin0[...] = n0[...].astype(BF16)
    work[...] = DOT(thin0[...], thin0[...], NN) - 2.0 * n0[...]
    term[...] = work[...].astype(BF16)
    term[...] = (DOT(term[...], term[...], NN) + 2.0 * work[...]).astype(BF16)
    n1[...] = 1.25**4 * (DOT(term[...], thin0[...], NN) + n0[...])
    thin1[...] = n1[...].astype(BF16)
    pair = DOT(thin[...], thin1[...], NN)
    corr[...] = pair[:B] - n0[...] - n1[...]
    work[...] = pair[B:] - 2.0 * n1[...]
    term[...] = work[...].astype(BF16)
    term[...] = (DOT(term[...], term[...], NN) + 2.0 * work[...]).astype(BF16)
    n0[...] = 1.25**4 * (DOT(term[...], thin1[...], NN) + n1[...])
    factor = 1.25**3 * lax.rsqrt(jnp.sqrt(jnp.sqrt(square)))
    inverse = corr[...] - n0[...] - DOT(corr[...].astype(BF16), n0[...].astype(BF16), NN)
    root[...] = (factor * (inverse + jnp.where(eye, 1.0, 0.0))).astype(BF16)

    @pl.when(team == 0)
    def _():
        wait(zs_end.at[pl.ds(0, NY - 1)], zs2r)
        wait(ys_end.at[pl.ds(0, NZ - 1)], ys2r)
        zs_end[y] = zs_mid[y // 2]
        ys_end[z] = ys_mid[z // 2]
        summed = jnp.concatenate([total(zs_end, NY), total(ys_end, NZ)], axis=0)
        both = DOT(stacked(summed), root[...], NN)
        turned = both[:COLS] + both[COLS:]
        lane = lax.broadcasted_iota(jnp.int32, (8, T), 1) // COLS
        for e in range(NT):
            tile = jnp.zeros((8, T), F32)
            for q in range(NB):
                part = turned[8 * q : 8 * q + 8, T * (e // NB) : T * (e // NB) + T]
                shift = (COLS * (q - e % NB)) % T
                tile = jnp.where(lane == q, pltpu.roll(part, shift, 1) if shift else part, tile)
            t_send[8 * e : 8 * e + 8, :] = tile

        for dy, dh in pairs_of(NY, NZ // 2):
            e = ys[dy] * (NZ // 2) + halves[dh]
            send(
                t_send.at[pl.ds(pl.multiple_of(8 * e, 8), 8), :],
                t_buf.at[pl.ds(pl.multiple_of(8 * member, 8), 8), :],
                ts, tr, at(y=ys[dy], z=2 * halves[dh] + lax.rem(1 + ys[dy], 2)),
            )

        ea_send[...] = jnp.zeros((1, T), F32)

    @pl.when(team == 1)
    def _():
        wait(t_buf, tr)

    @pl.when(team == 1)
    def _():
        turned = t_buf[...].T
        rows = jnp.concatenate([turned[COLS * q : COLS * (q + 1), :] for q in range(NB)], axis=1)
        both = DOT(stacked(rows), root[...], NN)
        p_all[...] = (both[:COLS] + both[COLS:]) * (1.0 / NP)
        lane = lax.broadcasted_iota(jnp.int32, (1, T), 1)
        energy = jnp.sum(p_all[...] * p_all[...], axis=(0, 1), keepdims=True)
        here = layer_ref[0]
        ea_send[...] = jnp.where(lane == here, energy, 0.0) + jnp.where(
            lane == here + LAYERS, float(COLS * B), 0.0
        )

    place = (y * NH + h) * NC + c
    ea_buf[place] = ea_send[...]

    for hh in (1 - h, h):
        for dy in spread(NY):
            for cc in (1 - c, c):
                if not (hh is h and cc is c and dy == 0):
                    send(ea_send, ea_buf.at[place], eas, ear, at(y=ys[dy], h=hh, c=cc))

    @pl.when(team == 1)
    def _():
        partner = z + 1 - 2 * (z % 2)
        send(
            p_all.at[pl.ds(pl.multiple_of(ROWS * (partner % 2), ROWS), ROWS), :],
            p_buf, ps, pr, at(z=partner),
        )
        p_buf[...] = p_all[pl.ds(pl.multiple_of(ROWS * (z % 2), ROWS), ROWS), :]

    wait(ea_buf.at[pl.ds(0, NY * NH * NC - 1)], ear)
    eb_send[...] = jnp.sum(ea_buf[...], axis=0)
    spot = x * NZ + z
    eb_buf[spot] = eb_send[...]

    for dx, dz in pairs_of(NX, NZ)[:-1]:
        send(eb_send, eb_buf.at[spot], ebs, ebr, at(x=xs[dx], z=zs[dz]))

    @pl.when(team == 0)
    def _():
        wait(p_buf, pr)

    wait(eb_buf.at[pl.ds(0, NX * NZ - 1)], ebr)
    sums = jnp.sum(eb_buf[...], axis=0)
    lane = lax.broadcasted_iota(jnp.int32, (1, T), 1)
    here = layer_ref[0]
    layer_square = jnp.sum(jnp.where(lane == here, sums, 0.0), axis=1, keepdims=True)
    layer_count = jnp.sum(jnp.where(lane == here + LAYERS, sums, 0.0), axis=1, keepdims=True)
    out_ref[0] = (p_buf[...] * lax.rsqrt(layer_square / layer_count + 1e-06)).astype(BF16)

    for ref, count, sem in (
        (y_buf, NY, y1s), (z_buf, NZ, z1s), (z_end, NY, z2s), (y_end, NZ, y2s), (ag_buf, NT, ags),
        (ys_buf, NY, ys1s), (zs_buf, NZ, zs1s), (ea_buf, NY * NH * NC, eas), (eb_buf, NX * NZ, ebs),
    ):
        wait(ref.at[pl.ds(0, count - 1)], sem)
    wait(zs_mid.at[pl.ds(0, NY // 2 - 1)], zs2s)
    wait(ys_mid.at[pl.ds(0, NZ // 2 - 1)], ys2s)

    @pl.when(team == 0)
    def _():
        wait(t_send, ts)

    @pl.when(team == 1)
    def _():
        wait(zs_mid.at[0], zs2s)
        wait(ys_mid.at[0], ys2s)
        wait(p_buf, ps)


def per_device(gradients, block_layer):
    return pl.pallas_call(
        body,
        out_shape=pltpu.VMEM((1, ROWS, B), BF16),
        in_specs=[
            pl.BlockSpec(memory_space=pltpu.HBM),
            pl.BlockSpec(memory_space=pltpu.HBM),
        ],
        out_specs=pl.BlockSpec(memory_space=pltpu.VMEM),
        scratch_shapes=[
            pltpu.VMEM((B, B), BF16),
            pltpu.VMEM((B, B), F32),
            pltpu.VMEM((2, PACKED, T), F32),
            pltpu.VMEM((NZ, NY, VIA_Z, T), BF16),
            pltpu.VMEM((NY, NZ, VIA_Y, T), BF16),
            pltpu.VMEM((NZ, NY, VIA_Z, T), BF16),
            pltpu.VMEM((NY, NZ, VIA_Y, T), BF16),
            pltpu.VMEM((NY, VIA_Z, T), BF16),
            pltpu.VMEM((NZ, VIA_Y, T), BF16),
            pltpu.VMEM((NY, VIA_Z, T), BF16),
            pltpu.VMEM((NZ, VIA_Y, T), BF16),
            pltpu.VMEM((CHUNK, T), BF16),
            pltpu.VMEM((NT, CHUNK, T), BF16),
            pltpu.VMEM((NZ, NY // 2, COLS // 2, B), BF16),
            pltpu.VMEM((NY, NZ // 2, COLS // 2, B), BF16),
            pltpu.VMEM((NZ, NY // 2, COLS // 2, B), BF16),
            pltpu.VMEM((NY, NZ // 2, COLS // 2, B), BF16),
            pltpu.VMEM((NY // 2, COLS // 2, B), F32),
            pltpu.VMEM((NZ // 2, COLS // 2, B), F32),
            pltpu.VMEM((NY, COLS // 2, B), F32),
            pltpu.VMEM((NZ, COLS // 2, B), F32),
        ]
        + [pltpu.VMEM((B, B), F32)] * 4
        + [
            pltpu.VMEM((2 * B, B), BF16),
            pltpu.VMEM((B, B), BF16),
            pltpu.VMEM((B, B), BF16),
            pltpu.VMEM((8 * NT, T), F32),
            pltpu.VMEM((8 * NT, T), F32),
            pltpu.VMEM((COLS, B), F32),
            pltpu.VMEM((ROWS, B), F32),
            pltpu.VMEM((1, T), F32),
            pltpu.VMEM((NY * NH * NC, 1, T), F32),
            pltpu.VMEM((1, T), F32),
            pltpu.VMEM((NX * NZ, 1, T), F32),
            pltpu.SMEM((1,), jnp.int32),
            pltpu.SemaphoreType.DMA((28,)),
        ],
        compiler_params=pltpu.CompilerParams(
            collective_id=0, has_side_effects=True, vmem_limit_bytes=60 * 1024 * 1024,
        ),
    )(gradients, block_layer)


def solution(mesh):
    finer = Mesh(mesh.devices.reshape(NY, NZ, NX, NH, NC), AXES)
    return jax.shard_map(
        per_device,
        mesh=finer,
        in_specs=(P(("y", "z"), ("x", "h", "c"), None, None), P(("x", "h", "c"))),
        out_specs=P(("x", "h", "c"), ("y", "z"), None),
        check_vma=False,
    )
```
